32 devices in a mesh: face: 2 (over y), fy: 4 (over x, core), fx: 4 (over z).
Axes of the slice: x: 2, y: 2, z: 4, core: 2. Of those that a mesh axis runs over, the one named last changes fastest.
Arguments:
- state: float32 [6, 32, 32, 192], P('face', 'fy', 'fx'), may hold values from -6 to 6
- jacobian: float32 [6, 32, 32], P('face', 'fy', 'fx'), may hold values from 0.5 to 2
- metric_diag: float32 [2, 6, 32, 32], P(None, 'face', 'fy', 'fx'), may hold values from 0.6 to 1.4
- metric_cross: float32 [6, 32, 32], P('face', 'fy', 'fx'), may hold values from -0.3 to 0.3
- coriolis: float32 [6, 32, 32], P('face', 'fy', 'fx'), may hold values from -2 to 2
- nbr_face: int32 [6, 4], replicated, may hold values from 0 to 5, as said below
- nbr_edge: int32 [6, 4], replicated, may hold values from 0 to 3, as said below
Outputs:
- updated: float32 [6, 32, 32, 192], P('face', 'fy', 'fx')
The draws below stay inside these ranges and needn't reach their ends.
Inputs may be any that keep to these rules, and one draw needn't show every extreme that they name: Edge e of a face is 0 south (row 0), 1 east (last column), 2 north (last row), 3 west (column 0). Edge e of face f is glued to edge nbr_edge[f, e] of face nbr_face[f, e], and that edge back to it; the 6 faces are glued as the surface of a cube, three faces at each corner, the two glued edges running in opposite senses when both are read counterclockwise. `nbr_edge`: see nbr_face.
All inputs are finite; a program needn't handle non-finite values.
Results may differ from the reference program's by a relative error of at most 0.0001.
Values sent between devices are 32-bit elements; how exact they have to be, the bound alone decides.
A program may use at most 64 MiB of HBM per device.

```python
import math
import jax
import jax.numpy as jnp
import numpy as np
from jax import lax

FACES = 6
LEV = 64
NN = 32


def glued_tables(key):
    base_key = jax.random.fold_in(key, 4051)
    relabel = jax.random.permutation(jax.random.fold_in(base_key, 1), 6).astype(jnp.int32)
    quarter = jax.random.randint(jax.random.fold_in(base_key, 2), (6,), 0, 4).astype(jnp.int32)
    drawn_face = jnp.asarray(np.array([[5, 1, 4, 3], [5, 2, 4, 0], [5, 3, 4, 1], [5, 0, 4, 2], [0, 1, 2, 3], [2, 1, 0, 3]]), jnp.int32)
    drawn_edge = jnp.asarray(np.array([[2, 3, 0, 1], [1, 3, 1, 1], [0, 3, 2, 1], [3, 3, 3, 1], [2, 2, 2, 2], [0, 0, 0, 0]]), jnp.int32)
    old_face = jnp.broadcast_to(jnp.arange(6, dtype=jnp.int32)[:, None], (6, 4))
    old_edge = jnp.broadcast_to(jnp.arange(4, dtype=jnp.int32)[None, :], (6, 4))
    new_face = relabel[old_face]
    new_edge = (old_edge + quarter[old_face]) % 4
    glued_face = relabel[drawn_face]
    glued_edge = (drawn_edge + quarter[drawn_face]) % 4
    faces_out = jnp.zeros((6, 4), jnp.int32).at[new_face, new_edge].set(glued_face)
    edges_out = jnp.zeros((6, 4), jnp.int32).at[new_face, new_edge].set(glued_edge)
    return (faces_out, edges_out)


def draw_nbr_face(key, part):
    return glued_tables(key)[0]


def draw_nbr_edge(key, part):
    return glued_tables(key)[1]


def level_of(key, shape, pieces, smallest, top_value):
    gain, own = 1.0, jax.random.fold_in(key, 6)
    for axis_at, blocks in pieces:
        draws = jnp.exp(jax.random.uniform(jax.random.fold_in(own, axis_at), (blocks,), jnp.float32, smallest / len(pieces), top_value / len(pieces)))
        gain = gain * jnp.repeat(draws, shape[axis_at] // blocks).reshape([-1 if axis == axis_at else 1 for axis in range(len(shape))])
    return gain


def bell_draw(key, dims, scale, most, split=(), held_as=jnp.bfloat16):
    level = level_of(key, dims, split, -0.22, 0.18) if split else 1.0
    values = jax.random.normal(key, dims, jnp.float32) * scale * level
    return jnp.minimum(jnp.maximum(values, -most), most).astype(held_as)


def setup_inputs(seed: int = 0) -> dict:
    splits = jax.random.split(jax.random.key(seed), 8)
    return {
        "state": bell_draw(splits[0], (FACES, NN, NN, 3 * LEV), 1.0, 6.0, ((0, 2), (1, 4), (2, 4)), jnp.float32),
        "jacobian": jnp.clip(jnp.exp(math.log(2.0) - 1.3862944 * jax.random.uniform(splits[1], (FACES, NN, NN), jnp.float32) ** level_of(splits[1], (FACES, NN, NN), ((0, 2), (1, 4), (2, 4)), -0.2, 0.2)), 0.5, 2.0),
        "metric_diag": jnp.clip(1.0 + 0.08 * jax.random.normal(splits[2], (2, FACES, NN, NN), jnp.float32), 0.6, 1.4),
        "metric_cross": jnp.clip(jax.random.uniform(splits[3], (FACES, NN, NN), jnp.float32, -0.3, 0.3) * level_of(splits[3], (FACES, NN, NN), ((0, 2), (1, 4), (2, 4)), -0.4, 0.0), -0.3, 0.3),
        "coriolis": jnp.clip(jax.random.uniform(splits[4], (FACES, NN, NN), jnp.float32, -2.0, 2.0) * level_of(splits[4], (FACES, NN, NN), ((0, 2), (1, 4), (2, 4)), -0.4, 0.0), -2.0, 2.0),
        "nbr_face": draw_nbr_face(jax.random.fold_in(splits[7], 71), 0),
        "nbr_edge": draw_nbr_edge(jax.random.fold_in(splits[7], 71), 0),
    }


time_step = 0.05
hyper_coeff = 0.0005

def deriv_table():
    gll_nodes = np.array([-1.0, -1.0 / np.sqrt(5.0), 1.0 / np.sqrt(5.0), 1.0])
    bary_weights = np.ones(4)
    for j in range(4):
        for m in range(4):
            if m != j:
                bary_weights[j] = bary_weights[j] / (gll_nodes[j] - gll_nodes[m])
    matrix = np.zeros((4, 4))
    for i in range(4):
        for j in range(4):
            if i != j:
                matrix[i, j] = bary_weights[j] / bary_weights[i] / (gll_nodes[i] - gll_nodes[j])
        matrix[i, i] = -np.sum(matrix[i])
    return matrix

def along_x(values):
    face_count, row_count, col_count, chan_count = values.shape
    blocks = values.reshape(face_count, row_count, col_count // 4, 4, chan_count)
    result = jnp.einsum('jk,abekc->abejc', jnp.asarray(deriv_table(), jnp.float32), blocks, precision=lax.Precision.HIGHEST)
    return result.reshape(values.shape)

def along_y(values):
    face_count, row_count, col_count, chan_count = values.shape
    blocks = values.reshape(face_count, row_count // 4, 4, col_count, chan_count)
    result = jnp.einsum('ik,aekxc->aeixc', jnp.asarray(deriv_table(), jnp.float32), blocks, precision=lax.Precision.HIGHEST)
    return result.reshape(values.shape)

def mass_of(jacobian):
    weights = jnp.asarray([1.0 / 6.0, 5.0 / 6.0, 5.0 / 6.0, 1.0 / 6.0], jnp.float32)
    row_weight = jnp.tile(weights, jacobian.shape[1] // 4)
    col_weight = jnp.tile(weights, jacobian.shape[2] // 4)
    return jacobian * row_weight[None, :, None] * col_weight[None, None, :]

def tendency(state, geometry, planet):
    volume, metric_xx, metric_yy, metric_xy = geometry
    levels = state.shape[-1] // 3
    wind_u = state[..., :levels]
    wind_v = state[..., levels:2 * levels]
    temper = state[..., 2 * levels:]
    contra_u = metric_xx * wind_u + metric_xy * wind_v
    contra_v = metric_xy * wind_u + metric_yy * wind_v
    energy = 0.5 * (wind_u * contra_u + wind_v * contra_v) + temper
    xderivs = along_x(jnp.concatenate([wind_v, temper, energy], -1))
    yderivs = along_y(jnp.concatenate([wind_u, temper, energy], -1))
    absolute = (xderivs[..., :levels] - yderivs[..., :levels]) / volume + planet
    tend_u = absolute * volume * contra_v - xderivs[..., 2 * levels:]
    tend_v = -absolute * volume * contra_u - yderivs[..., 2 * levels:]
    tend_t = -(contra_u * xderivs[..., levels:2 * levels] + contra_v * yderivs[..., levels:2 * levels])
    return state + time_step * jnp.concatenate([tend_u, tend_v, tend_t], -1)

def laplace(values, geometry):
    volume, metric_xx, metric_yy, metric_xy = geometry
    grad_x = along_x(values)
    grad_y = along_y(values)
    flux_x = volume * (metric_xx * grad_x + metric_xy * grad_y)
    flux_y = volume * (metric_xy * grad_x + metric_yy * grad_y)
    return (along_x(flux_x) + along_y(flux_y)) / volume

def combine(values, axis):
    length = values.shape[axis] - 2
    positions = jnp.arange(length)
    leading = (positions % 4 == 0).astype(jnp.float32)
    trailing = (positions % 4 == 3).astype(jnp.float32)
    broad_shape = [1, 1, 1, 1]
    broad_shape[axis] = length
    leading = leading.reshape(broad_shape)
    trailing = trailing.reshape(broad_shape)
    middle = lax.slice_in_dim(values, 1, length + 1, axis=axis)
    previous = lax.slice_in_dim(values, 0, length, axis=axis)
    following = lax.slice_in_dim(values, 2, length + 2, axis=axis)
    return middle + leading * previous + trailing * following

def rotate(segment, quarter, levels):
    cosine = ((quarter == 0).astype(jnp.float32) - (quarter == 2).astype(jnp.float32))[..., None]
    sine_part = ((quarter == 1).astype(jnp.float32) - (quarter == 3).astype(jnp.float32))[..., None]
    wind_u = segment[..., :levels]
    wind_v = segment[..., levels:2 * levels]
    return jnp.concatenate([cosine * wind_u - sine_part * wind_v, sine_part * wind_u + cosine * wind_v, segment[..., 2 * levels:]], -1)

def assemble(values, vector, nbr_face, nbr_edge):
    padded = jnp.pad(values, ((0, 0), (1, 1), (1, 1), (0, 0)))
    summed = combine(combine(padded, 1), 2)
    side_nodes = summed.shape[1]
    levels = summed.shape[-1] // 3
    rim_strips = jnp.stack([summed[:, 0, :], summed[:, :, side_nodes - 1], summed[:, side_nodes - 1, ::-1], summed[:, ::-1, 0]], axis=1)
    partner = rim_strips[nbr_face, nbr_edge][:, :, ::-1]
    if vector:
        quarter = (jnp.arange(4, dtype=jnp.int32)[None, :] - nbr_edge + 2) % 4
        partner = rotate(partner, quarter[:, :, None], levels)
    result = summed.at[:, 0, :].add(partner[:, 0])
    result = result.at[:, :, side_nodes - 1].add(partner[:, 1])
    result = result.at[:, side_nodes - 1, :].add(partner[:, 2, ::-1])
    result = result.at[:, :, 0].add(partner[:, 3, ::-1])
    return result

def reference(state, jacobian, metric_diag, metric_cross, coriolis, nbr_face, nbr_edge):
    node_mass = mass_of(jacobian)[..., None]
    total_mass = assemble(node_mass, False, nbr_face, nbr_edge)
    geometry = (jacobian[..., None], metric_diag[0][..., None], metric_diag[1][..., None], metric_cross[..., None])
    raw = tendency(state, geometry, coriolis[..., None])
    sectioned = assemble(node_mass * raw, True, nbr_face, nbr_edge) / total_mass
    first_lap = assemble(node_mass * laplace(sectioned, geometry), True, nbr_face, nbr_edge) / total_mass
    second_lap = assemble(node_mass * laplace(first_lap, geometry), True, nbr_face, nbr_edge) / total_mass
    return sectioned - hyper_coeff * second_lap
```

```python
import functools

import jax
import jax.numpy as jnp
import numpy as np
from jax import lax
from jax.experimental import pallas as pl
from jax.experimental.pallas import tpu as pltpu
from jax.sharding import PartitionSpec as P

time_step = 0.05
hyper_coeff = 0.0005
MESH = pl.DeviceIdType.MESH


def padded(cells, sides, width):
    for axis, dim in sides:
        count = lax.axis_size(axis)
        ends = count - 1
        head = lax.slice_in_dim(cells, 0, width, axis=dim)
        tail = lax.slice_in_dim(cells, cells.shape[dim] - width, cells.shape[dim], axis=dim)
        cells = jnp.concatenate(
            [
                lax.ppermute(tail, axis, [(i, (i + 1) % count) for i in range(ends)]),
                cells,
                lax.ppermute(head, axis, [((i + 1) % count, i) for i in range(ends)]),
            ],
            axis=dim,
        )
    return cells


def deriv_table():
    gll_nodes = np.array([-1.0, -1.0 / np.sqrt(5.0), 1.0 / np.sqrt(5.0), 1.0])
    bary_weights = np.ones(4)
    for j in range(4):
        for m in range(4):
            if m != j:
                bary_weights[j] = bary_weights[j] / (gll_nodes[j] - gll_nodes[m])
    matrix = np.zeros((4, 4))
    for i in range(4):
        for j in range(4):
            if i != j:
                matrix[i, j] = bary_weights[j] / bary_weights[i] / (gll_nodes[i] - gll_nodes[j])
        matrix[i, i] = -np.sum(matrix[i])
    return matrix


def along_x(values):
    face_count, row_count, col_count, chan_count = values.shape
    blocks = values.reshape(face_count, row_count, col_count // 4, 4, chan_count)
    result = jnp.einsum(
        "jk,abekc->abejc",
        jnp.asarray(deriv_table(), jnp.float32),
        blocks,
        precision=lax.Precision.HIGHEST,
    )
    return result.reshape(values.shape)


def along_y(values):
    face_count, row_count, col_count, chan_count = values.shape
    blocks = values.reshape(face_count, row_count // 4, 4, col_count, chan_count)
    result = jnp.einsum(
        "ik,aekxc->aeixc",
        jnp.asarray(deriv_table(), jnp.float32),
        blocks,
        precision=lax.Precision.HIGHEST,
    )
    return result.reshape(values.shape)


def mass_of(jacobian):
    weights = jnp.asarray([1.0 / 6.0, 5.0 / 6.0, 5.0 / 6.0, 1.0 / 6.0], jnp.float32)
    row_weight = jnp.tile(weights, jacobian.shape[1] // 4)
    col_weight = jnp.tile(weights, jacobian.shape[2] // 4)
    return jacobian * row_weight[None, :, None] * col_weight[None, None, :]


def tendency(state, geometry, planet):
    volume, metric_xx, metric_yy, metric_xy = geometry
    levels = state.shape[-1] // 3
    wind_u = state[..., :levels]
    wind_v = state[..., levels : 2 * levels]
    temper = state[..., 2 * levels :]
    contra_u = metric_xx * wind_u + metric_xy * wind_v
    contra_v = metric_xy * wind_u + metric_yy * wind_v
    energy = 0.5 * (wind_u * contra_u + wind_v * contra_v) + temper
    xderivs = along_x(jnp.concatenate([wind_v, temper, energy], -1))
    yderivs = along_y(jnp.concatenate([wind_u, temper, energy], -1))
    absolute = (xderivs[..., :levels] - yderivs[..., :levels]) / volume + planet
    tend_u = absolute * volume * contra_v - xderivs[..., 2 * levels :]
    tend_v = -absolute * volume * contra_u - yderivs[..., 2 * levels :]
    tend_t = -(
        contra_u * xderivs[..., levels : 2 * levels] + contra_v * yderivs[..., levels : 2 * levels]
    )
    return state + time_step * jnp.concatenate([tend_u, tend_v, tend_t], -1)


def laplace(values, geometry):
    volume, metric_xx, metric_yy, metric_xy = geometry
    grad_x = along_x(values)
    grad_y = along_y(values)
    flux_x = volume * (metric_xx * grad_x + metric_xy * grad_y)
    flux_y = volume * (metric_xy * grad_x + metric_yy * grad_y)
    return (along_x(flux_x) + along_y(flux_y)) / volume


def combine(values, axis):
    length = values.shape[axis] - 2
    positions = jnp.arange(length)
    leading = (positions % 4 == 0).astype(jnp.float32)
    trailing = (positions % 4 == 3).astype(jnp.float32)
    broad_shape = [1, 1, 1, 1]
    broad_shape[axis] = length
    leading = leading.reshape(broad_shape)
    trailing = trailing.reshape(broad_shape)
    middle = lax.slice_in_dim(values, 1, length + 1, axis=axis)
    previous = lax.slice_in_dim(values, 0, length, axis=axis)
    following = lax.slice_in_dim(values, 2, length + 2, axis=axis)
    return middle + leading * previous + trailing * following


def rotate(segment, quarter, levels):
    cosine = ((quarter == 0).astype(jnp.float32) - (quarter == 2).astype(jnp.float32))[..., None]
    sine_part = ((quarter == 1).astype(jnp.float32) - (quarter == 3).astype(jnp.float32))[..., None]
    wind_u = segment[..., :levels]
    wind_v = segment[..., levels : 2 * levels]
    return jnp.concatenate(
        [
            cosine * wind_u - sine_part * wind_v,
            sine_part * wind_u + cosine * wind_v,
            segment[..., 2 * levels :],
        ],
        -1,
    )


def in_face(values):
    across = combine(padded(values, (("fx", 2),), 1), 2)
    return combine(padded(across, (("fy", 1),), 1), 1)


def place_pieces(
    got_flat,
    got_tall,
    vector,
    nbr_edge,
    flat_edge,
    tall_edge,
    on_south,
    on_west,
    flat_start,
    tall_start,
    face_local,
    side_nodes,
    chan_count,
    levels,
):
    edge_ids = jnp.arange(4, dtype=jnp.int32)
    flat_target = nbr_edge[:, flat_edge]
    tall_target = nbr_edge[:, tall_edge]
    if vector:
        got_flat = rotate(got_flat, ((flat_target - flat_edge + 2) % 4)[None, :, None], levels)
        got_tall = rotate(got_tall, ((tall_target - tall_edge + 2) % 4)[None, :, None], levels)
    got_flat = jnp.where(on_south, got_flat[:, :, ::-1], got_flat)
    got_tall = jnp.where(on_west, got_tall, got_tall[:, :, ::-1])
    flat_pick = (flat_target[:, None] == edge_ids[None, :]).astype(jnp.float32)
    tall_pick = (tall_target[:, None] == edge_ids[None, :]).astype(jnp.float32)
    flat_rims = jnp.einsum("se,gsjc->gejc", flat_pick, got_flat, precision=lax.Precision.HIGHEST)
    tall_rims = jnp.einsum("se,gsjc->gejc", tall_pick, got_tall, precision=lax.Precision.HIGHEST)
    empty_rims = jnp.zeros((face_local, 4, side_nodes, chan_count), jnp.float32)
    rim_strips = lax.dynamic_update_slice(empty_rims, flat_rims, (0, 0, flat_start, 0))
    return rim_strips + lax.dynamic_update_slice(empty_rims, tall_rims, (0, 0, tall_start, 0))


def outgoing(
    summed, nbr_face, face_ids, flat_edge, tall_edge, on_south, on_west, flat_live, tall_live
):
    row_count = summed.shape[1]
    col_count = summed.shape[2]
    all_faces = jnp.arange(nbr_face.shape[0], dtype=jnp.int32)
    flat_piece = jnp.where(on_south, summed[:, 0], summed[:, row_count - 1])
    tall_piece = jnp.where(on_west, summed[:, :, 0], summed[:, :, col_count - 1])
    flat_dest = nbr_face[face_ids, flat_edge]
    tall_dest = nbr_face[face_ids, tall_edge]
    flat_send = ((all_faces[:, None] == flat_dest[None, :]) & flat_live).astype(jnp.float32)
    tall_send = ((all_faces[:, None] == tall_dest[None, :]) & tall_live).astype(jnp.float32)
    return (
        flat_send[:, :, None, None] * flat_piece[None],
        tall_send[:, :, None, None] * tall_piece[None],
    )


def assemble(values, vector, nbr_face, nbr_edge):
    summed = in_face(values)
    face_local, row_count, col_count, chan_count = summed.shape
    levels = chan_count // 3
    row_index = lax.axis_index("fy")
    col_index = lax.axis_index("fx")
    side_nodes = row_count * lax.axis_size("fy")
    face_ids = lax.axis_index("face") * face_local + jnp.arange(face_local, dtype=jnp.int32)
    on_south = row_index == 0
    on_north = row_index == lax.axis_size("fy") - 1
    on_west = col_index == 0
    on_east = col_index == lax.axis_size("fx") - 1
    flat_live = on_south | on_north
    tall_live = on_west | on_east
    flat_edge = jnp.where(on_south, 0, 2).astype(jnp.int32)
    tall_edge = jnp.where(on_west, 3, 1).astype(jnp.int32)
    flat_start = jnp.where(
        on_south, side_nodes - (col_index + 1) * col_count, col_index * col_count
    )
    tall_start = jnp.where(on_west, row_index * row_count, side_nodes - (row_index + 1) * row_count)
    send_flat, send_tall = outgoing(
        summed, nbr_face, face_ids, flat_edge, tall_edge, on_south, on_west, flat_live, tall_live
    )
    got_flat, got_tall = (
        lax.all_to_all(send_flat, "face", split_axis=0, concat_axis=1, tiled=True),
        lax.all_to_all(send_tall, "face", split_axis=0, concat_axis=1, tiled=True),
    )
    rim_strips = place_pieces(
        got_flat,
        got_tall,
        vector,
        nbr_edge,
        flat_edge,
        tall_edge,
        on_south,
        on_west,
        flat_start,
        tall_start,
        face_local,
        side_nodes,
        chan_count,
        levels,
    )
    flat_lines = jnp.stack([rim_strips[:, 0], rim_strips[:, 2, ::-1]], axis=1)
    flat_lines = flat_lines.reshape(face_local, 2, lax.axis_size("fx"), col_count, chan_count)
    tall_lines = jnp.stack([rim_strips[:, 1], rim_strips[:, 3, ::-1]], axis=1)
    tall_lines = tall_lines.reshape(face_local, 2, lax.axis_size("fy"), row_count, chan_count)
    flat_whole = lax.psum(flat_lines, "fy")
    tall_whole = lax.psum(tall_lines, "fx")
    flat_block = lax.psum_scatter(flat_whole, "fx", scatter_dimension=2, tiled=True)
    tall_block = lax.psum_scatter(tall_whole, "fy", scatter_dimension=2, tiled=True)
    flat_add = jnp.where(on_south, flat_block[:, 0, 0], flat_block[:, 1, 0])
    tall_add = jnp.where(on_west, tall_block[:, 1, 0], tall_block[:, 0, 0])
    result = summed.at[:, 0].add(jnp.where(on_south, flat_add, 0.0))
    result = result.at[:, row_count - 1].add(jnp.where(on_north, flat_add, 0.0))
    result = result.at[:, :, 0].add(jnp.where(on_west, tall_add, 0.0))
    result = result.at[:, :, col_count - 1].add(jnp.where(on_east, tall_add, 0.0))
    return result


def per_device(state, jacobian, metric_diag, metric_cross, coriolis, nbr_face, nbr_edge):
    node_mass = mass_of(jacobian)[..., None]
    total_mass = assemble(node_mass, False, nbr_face, nbr_edge)
    geometry = (
        jacobian[..., None],
        metric_diag[0][..., None],
        metric_diag[1][..., None],
        metric_cross[..., None],
    )
    raw = tendency(state, geometry, coriolis[..., None])
    sectioned = assemble(node_mass * raw, True, nbr_face, nbr_edge) / total_mass
    first_lap = (
        assemble(node_mass * laplace(sectioned, geometry), True, nbr_face, nbr_edge) / total_mass
    )
    second_lap = (
        assemble(node_mass * laplace(first_lap, geometry), True, nbr_face, nbr_edge) / total_mass
    )
    return sectioned - hyper_coeff * second_lap


SIDE = 8
HALF = 64
LANES = 128


def widen(ref, index, r):
    row = jnp.broadcast_to(ref[index + (pl.ds(r, 1), slice(None))].reshape(1, SIDE), (SIDE, SIDE))
    eye = lax.broadcasted_iota(jnp.int32, (SIDE, SIDE), 0) == lax.broadcasted_iota(jnp.int32, (SIDE, SIDE), 1)
    return jnp.broadcast_to(jnp.sum(jnp.where(eye, row, 0.0), axis=1, keepdims=True), (SIDE, LANES))


def up(v, count, axis):
    return pltpu.roll(v, v.shape[axis] - count, axis)


def down(v, count, axis):
    return pltpu.roll(v, count, axis)


def slope(a):
    d = deriv_table()
    p0, p1, m0, m1 = a[0] + a[3], a[1] + a[2], a[0] - a[3], a[1] - a[2]
    bend = p0 - p1
    o0 = jnp.float32((d[0, 0] + d[0, 3]) / 2) * bend
    o1 = jnp.float32((d[1, 0] + d[1, 3]) / 2) * bend
    q0 = jnp.float32((d[0, 0] - d[0, 3]) / 2) * m0 + jnp.float32((d[0, 1] - d[0, 2]) / 2) * m1
    q1 = jnp.float32((d[1, 0] - d[1, 3]) / 2) * m0 + jnp.float32((d[1, 1] - d[1, 2]) / 2) * m1
    return [q0 + o0, q1 + o1, q1 - o1, q0 - o0]


def slope_x(v):
    return [slope(v[i]) for i in range(4)]


def slope_y(v):
    cols = [slope([v[i][j] for i in range(4)]) for j in range(4)]
    return [[cols[j][i] for j in range(4)] for i in range(4)]


def element_rows(mix, er, i, which):
    start = er * 64 + which * 16 + i * 4
    return mix.at[pl.ds(start, 4)], mix.at[pl.ds(start + 32, 4)]


def spread(mix, plane, er, i, which, v):
    for ec in range(2):
        mix[plane, pl.ds(er * 64 + ec * 32 + which * 16 + i * 4, 4), :] = v[4 * ec : 4 * ec + 4]


def by_node(mix, plane):
    return jnp.concatenate([mix[plane, pl.ds(n, 8, stride=16), :] for n in range(16)], axis=0)


def main_kernel(
    groups,
    blocks,
    nbr_face,
    nbr_edge,
    state,
    jac,
    diag,
    cross,
    coriolis,
    out,
    mix,
    send,
    send_geo,
    got,
    got_geo,
    coef,
    section,
    back,
    sem_s_geo,
    sem_r_geo,
    sem_s_in,
    sem_r_in,
    sem_s_out,
    sem_r_out,
    sem_own,
):
    faces = state.shape[0]
    count = groups * blocks * blocks
    last = blocks - 1
    g = lax.axis_index("face")
    y = lax.axis_index("fy")
    x = lax.axis_index("fx")
    me = (g * blocks + y) * blocks + x

    def others():
        for dx in (2, 3, 1, 0):
            for dy in range(blocks):
                for dg in range(groups):
                    if dx or dy or dg:
                        at = (lax.rem(g + dg, groups), lax.rem(y + dy, blocks), lax.rem(x + dx, blocks))
                        yield (at[0] * blocks + at[1]) * blocks + at[2], at

    barrier = pltpu.get_barrier_semaphore()
    for _, at in others():
        pl.semaphore_signal(barrier, inc=1, device_id=at, device_id_type=MESH)

    sub = lax.broadcasted_iota(jnp.int32, (SIDE, LANES), 0)
    lane = lax.broadcasted_iota(jnp.int32, (SIDE, LANES), 1)
    low = lane < HALF
    node = sub % 4
    table = deriv_table()
    weights = (1.0 / 6.0, 5.0 / 6.0, 5.0 / 6.0, 1.0 / 6.0)
    zero = jnp.zeros((SIDE, LANES), jnp.float32)

    def per_node(entries):
        total = jnp.full((SIDE, LANES), entries[0], jnp.float32)
        for j in range(1, 4):
            total = jnp.where(node == j, jnp.float32(entries[j]), total)
        return total

    col_weight = per_node(weights)
    taps = {
        s: per_node([float(table[j, j + s]) if 0 <= j + s < 4 else 0.0 for j in range(4)])
        for s in range(-3, 4)
    }

    def swap(v):
        return pltpu.roll(v, HALF, 1)

    def along_sub(v):
        total = taps[0] * v
        for s in (-3, -2, -1, 1, 2, 3):
            total = total + taps[s] * pltpu.roll(v, (-s) % SIDE, 0)
        return total

    second = (lane >= 32) & (lane < 64)
    geo = [[[None, None] for _ in range(SIDE)] for _ in range(faces)]
    for f in range(faces):
        for start in range(0, SIDE, 4):
            wind, temp, contra, energy, vol, cor, mass = [], [], [], [], [], [], []
            for r in range(start, start + 4):
                j = widen(jac, (f,), r)
                m_xx, m_yy, m_xy = widen(diag, (0, f), r), widen(diag, (1, f), r), widen(cross, (f,), r)
                w = state[f, r, :, 0 : 2 * HALF]
                t = state[f, r, :, 2 * HALF : 3 * HALF]
                t = jnp.concatenate([t, t], axis=1)
                c = jnp.where(low, m_xx, m_yy) * w + m_xy * swap(w)
                p = w * c
                wind.append(w)
                temp.append(t)
                contra.append(c)
                energy.append(0.5 * (p + swap(p)) + t)
                vol.append(j)
                cor.append(widen(coriolis, (f,), r))
                mass.append(j * (jnp.float32(weights[r % 4]) * col_weight))
                even = lane % 2 == 0
                geo[f][r][0] = jnp.where(even, j * m_xx, j * m_yy)
                geo[f][r][1] = jnp.where(even, j * m_xy, mass[-1])
            dxs = [along_sub(jnp.where(low, energy[i], wind[i])) for i in range(4)]
            dys = slope([jnp.where(low, wind[i], energy[i]) for i in range(4)])
            dxt = [along_sub(temp[i]) for i in range(4)]
            dyt = slope(temp)
            for i in range(4):
                dxv = jnp.where(low, swap(dxs[i]), dxs[i])
                dyu = jnp.where(low, dys[i], swap(dys[i]))
                spin = (dxv - dyu) + cor[i] * vol[i]
                spin = jnp.where(low, spin, -spin)
                tend = spin * swap(contra[i]) - jnp.where(low, dxs[i], dys[i])
                fresh = mass[i] * (wind[i] + time_step * tend)
                q = contra[i] * jnp.where(low, dxt[i], dyt[i])
                heat = mass[i] * (temp[i] - time_step * (q + swap(q)))
                er = start // 4
                spread(mix, f, er, i, 0, jnp.where(second, down(heat, 32, 1), fresh))
                spread(mix, f, er, i, 1, jnp.where(second, heat, up(fresh, 32, 1)))
    for r in range(SIDE):
        for h in range(2):
            v = geo[0][r][h]
            for f in range(1, faces):
                v = jnp.where(lane >= 2 * f, geo[f][r][h], v)
            spread(mix, faces, r // 4, r % 4, h, v)
    for f in range(faces):
        turned = by_node(mix, f).T
        for k, part in enumerate((0, 2, 1)):
            send[k * faces + f] = turned[part * count : (part + 1) * count]
    send_geo[...] = by_node(mix, faces).T[0:SIDE]

    er, ec, lev = sub // 4, (sub // 2) % 2, sub % 2
    lx, ly = lane % blocks, (lane // blocks) % blocks
    panel = lane // (blocks * blocks)
    er0, er1, ec0, ec1 = er == 0, er == 1, ec == 0, ec == 1
    x_lo, x_hi, y_lo, y_hi = lx == 0, lx == last, ly == 0, ly == last
    edge_at = (er0 & y_lo, er1 & x_hi, er0 & y_hi, er1 & x_lo)

    first_at = jnp.zeros((SIDE, LANES), jnp.int32)
    step_at, quarter_at = first_at, first_at
    for e in range(4):
        firsts, steps, quarters = first_at * 0, first_at * 0, first_at * 0
        for f in range(faces):
            for k in range(groups):
                nf = nbr_face[e, k * faces + f]
                ne = nbr_edge[e, k * faces + f]
                nl, ng = nf % faces, nf // faces
                tall = ne % 2
                step = 1 + tall * (blocks - 1)
                flips = jnp.where(ne >= 2, 0 if e < 2 else 1, 1 if e < 2 else 0)
                offset = jnp.where(ne == 2, last * blocks, jnp.where(ne == 1, last, 0))
                first = (nl * groups + ng) * (blocks * blocks) + offset + flips * (last * step)
                here = panel == f * groups + k
                firsts = jnp.where(here, first, firsts)
                steps = jnp.where(here, step * (1 - 2 * flips), steps)
                quarters = jnp.where(here, (e - ne + 2 + 4) % 4, quarters)
        first_at = jnp.where(edge_at[e], firsts, first_at)
        step_at = jnp.where(edge_at[e], steps, step_at)
        quarter_at = jnp.where(edge_at[e], quarters, quarter_at)
    source_at = first_at + step_at * jnp.where(er0, lx, ly)
    flipped = step_at < 0
    from_flat = (step_at == 1) | (step_at == -1)
    cosine = jnp.where(quarter_at == 0, 1.0, jnp.where(quarter_at == 2, -1.0, 0.0))
    sine = jnp.where(quarter_at == 1, 1.0, jnp.where(quarter_at == 3, -1.0, 0.0))

    def next_row(v):
        s = down(v, 4, 0)
        return jnp.where(er0, s, jnp.where(y_hi, zero, up(s, blocks, 1)))

    def prev_row(v):
        s = down(v, 4, 0)
        return jnp.where(er1, s, jnp.where(y_lo, zero, down(s, blocks, 1)))

    def next_col(v):
        return jnp.where(ec0, up(v, 2, 0), jnp.where(x_hi, zero, up(down(v, 2, 0), 1, 1)))

    def prev_col(v):
        return jnp.where(ec1, down(v, 2, 0), jnp.where(x_lo, zero, down(up(v, 2, 0), 1, 1)))

    def within(v):
        v = [list(row) for row in v]
        for j in range(4):
            a, b = v[0][j], v[3][j]
            v[0][j], v[3][j] = a + prev_row(b), b + next_row(a)
        for i in range(4):
            a, b = v[i][0], v[i][3]
            v[i][0], v[i][3] = a + prev_col(b), b + next_col(a)
        return v

    def rims(v):
        found = []
        for b in range(4):
            flat = jnp.where(y_hi, v[3][b], v[0][b])
            flat = jnp.where(er0 == y_hi, down(flat, 4, 0), flat)
            tall = jnp.where(x_hi, v[b][3], v[b][0])
            tall = jnp.where(ec0 == x_hi, jnp.where(x_hi, up(tall, 2, 0), down(tall, 2, 0)), tall)
            tall = jnp.where(er == ec, tall, down(tall, 4, 0))
            flat = jnp.take_along_axis(flat, source_at, axis=1, mode="promise_in_bounds")
            tall = jnp.take_along_axis(tall, source_at, axis=1, mode="promise_in_bounds")
            found.append(jnp.where(from_flat, flat, tall))
        partner = []
        for b in range(4):
            w = found[3 - b]
            w = jnp.where(ec0, up(w, 2, 0), down(w, 2, 0))
            partner.append(jnp.where(flipped, w, found[b]))
        return partner

    def add_rims(v, partner):
        for b in range(4):
            p = partner[b]
            s = down(p, 4, 0)
            v[0][b] = v[0][b] + jnp.where(edge_at[0], p, zero)
            v[3][b] = v[3][b] + jnp.where(er1 & y_hi, s, zero)
            q = jnp.where(er1, p, s)
            q = jnp.where(er == ec, q, jnp.where(er0, down(q, 2, 0), up(q, 2, 0)))
            v[b][0] = v[b][0] + jnp.where(ec0 & x_lo, q, zero)
            v[b][3] = v[b][3] + jnp.where(ec1 & x_hi, q, zero)
        return v

    def assemble_one(v):
        v = within(v)
        return add_rims(v, rims(v))

    def assemble_pair(u, v):
        u, v = within(u), within(v)
        pu, pv = rims(u), rims(v)
        tu = [cosine * a - sine * b for a, b in zip(pu, pv)]
        tv = [sine * a + cosine * b for a, b in zip(pu, pv)]
        return add_rims(u, tu), add_rims(v, tv)

    def grid(flat):
        return [[flat[8 * (4 * i + j) : 8 * (4 * i + j) + 8] for j in range(4)] for i in range(4)]

    def receive(ref, planes):
        blocks_in = [ref[p] for p in planes]
        blocks_in += [blocks_in[0]] * (LANES // count - len(blocks_in))
        return grid(jnp.concatenate(blocks_in, axis=0).T)

    def put(ref, k, v):
        for i in range(4):
            for j in range(4):
                ref[k, i, j] = v[i][j]

    def take(ref, k):
        return [[ref[k, i, j] for j in range(4)] for i in range(4)]

    def each(fn, *vs):
        return [[fn(*(v[i][j] for v in vs)) for j in range(4)] for i in range(4)]

    def copies(src_of, dst, sem_s, sem_r):
        for d, at in others():
            pltpu.make_async_remote_copy(
                src_ref=src_of(d),
                dst_ref=dst,
                send_sem=sem_s,
                recv_sem=sem_r,
                device_id=at,
                device_id_type=MESH,
            ).start()

    def all_of(ref, sem_s, sem_r):
        part = ref.at[:, pl.ds(0, count - 1)]
        return pltpu.make_async_remote_copy(
            src_ref=part,
            dst_ref=part,
            send_sem=sem_s,
            recv_sem=sem_r,
            device_id=(g, y, lax.rem(x + 1, blocks)),
            device_id_type=MESH,
        )

    pairs = 2 * faces
    pl.semaphore_wait(barrier, count - 1)
    copies(lambda d: send_geo.at[pl.ds(0, pairs)], got_geo.at[:, me], sem_s_geo, sem_r_geo)
    copies(lambda d: send.at[:, d], got.at[:, me], sem_s_in, sem_r_in)
    for q in range(pairs):
        got_geo[q, pl.ds(me, 1), :] = send_geo[pl.ds(q, 1), :]
    for q in range(3 * faces):
        got[q, pl.ds(me, 1), :] = send[q, pl.ds(me, 1), :]

    all_of(got_geo, sem_s_geo, sem_r_geo).wait_recv()
    for p in range(2):
        both = receive(got_geo, range(p, pairs, 2))
        put(coef, 2 * p, each(lambda v: jnp.where(lev == 0, v, down(v, 1, 0)), both))
        put(coef, 2 * p + 1, each(lambda v: jnp.where(lev == 1, v, up(v, 1, 0)), both))
    put(coef, 3, each(lambda v: 1.0 / v, assemble_one(take(coef, 3))))

    def fields_in(k):
        return receive(got, range(k * faces, (k + 1) * faces))

    def scaled(v):
        return each(lambda a, b: a * b, v, take(coef, 3))

    def laplace_of(v):
        a, b, c = take(coef, 0), take(coef, 1), take(coef, 2)
        gx, gy = slope_x(v), slope_y(v)
        fx = each(lambda p, q, m, n: m * p + n * q, gx, gy, a, b)
        fy = each(lambda p, q, m, n: m * p + n * q, gx, gy, b, c)
        total = each(lambda p, q: p + q, slope_x(fx), slope_y(fy))
        return [[jnp.float32(weights[i] * weights[j]) * total[i][j] for j in range(4)] for i in range(4)]

    def finish(k, v):
        done = each(lambda s, a: s - hyper_coeff * a, take(section, k), v)
        turned = jnp.concatenate([done[i][j] for i in range(4) for j in range(4)], axis=0).T
        for f in range(faces):
            back[k * faces + f] = turned[f * count : (f + 1) * count]

    def send_back(k, n):
        part = pl.ds(k * faces, n * faces)
        copies(lambda d: back.at[part, d], out.at[part, me], sem_s_out, sem_r_out)
        own = pltpu.make_async_copy(back.at[part, me], out.at[part, me], sem_own.at[k])
        own.start()
        return own

    all_of(got, sem_s_in, sem_r_in).wait_recv()
    heat = scaled(assemble_one(fields_in(2)))
    put(section, 2, heat)
    wind_u, wind_v = assemble_pair(fields_in(0), fields_in(1))
    put(section, 0, scaled(wind_u))
    put(section, 1, scaled(wind_v))
    heat = scaled(assemble_one(laplace_of(heat)))
    heat = scaled(assemble_one(laplace_of(heat)))
    finish(2, heat)
    own_t = send_back(2, 1)
    wind_u, wind_v = assemble_pair(laplace_of(take(section, 0)), laplace_of(take(section, 1)))
    wind_u, wind_v = assemble_pair(laplace_of(scaled(wind_u)), laplace_of(scaled(wind_v)))
    finish(0, scaled(wind_u))
    finish(1, scaled(wind_v))
    own_w = send_back(0, 2)
    all_of(got_geo, sem_s_geo, sem_r_geo).wait_send()
    all_of(got, sem_s_in, sem_r_in).wait_send()
    own_t.wait()
    own_w.wait()
    all_of(out, sem_s_out, sem_r_out).wait_send()
    all_of(out, sem_s_out, sem_r_out).wait_recv()


def last_kernel(got, out, mix):
    faces = out.shape[0]
    lane = lax.broadcasted_iota(jnp.int32, (SIDE, LANES), 1)
    even = (lane // 32) % 2 == 0
    for f in range(faces):
        u, v, t = (got[k * faces + f] for k in range(3))
        turned = jnp.concatenate([u, t, v, v], axis=0).T
        for n in range(16):
            mix[f, pl.ds(n, 8, stride=16), :] = turned[8 * n : 8 * n + 8]
        for r in range(SIDE):
            start = (r // 4) * 64 + (r % 4) * 4
            a, b = (
                jnp.concatenate([mix[f, pl.ds(start + h * 16 + ec * 32, 4), :] for ec in range(2)], axis=0)
                for h in range(2)
            )
            out[f, r, :, 0 : 2 * HALF] = jnp.where(even, a, down(b, 32, 1))
            out[f, r, :, 2 * HALF : 3 * HALF] = jnp.where(even, up(a, 32, 1), b)[:, 0:HALF]


def by_level(groups, blocks, state, jacobian, metric_diag, metric_cross, coriolis, nbr_face, nbr_edge):
    faces = state.shape[0]
    count = groups * blocks * blocks
    vmem, smem = pl.BlockSpec(memory_space=pltpu.VMEM), pl.BlockSpec(memory_space=pltpu.SMEM)
    piece = (3 * faces, count, LANES)
    cells = (4, 4, SIDE, LANES)
    dma = pltpu.SemaphoreType.DMA
    got = pl.pallas_call(
        functools.partial(main_kernel, groups, blocks),
        out_shape=jax.ShapeDtypeStruct(piece, jnp.float32),
        in_specs=[smem, smem] + [vmem] * 5,
        out_specs=pl.BlockSpec(memory_space=pltpu.HBM),
        scratch_shapes=[
            pltpu.VMEM((faces + 1, LANES, LANES), jnp.float32),
            pltpu.VMEM(piece, jnp.float32),
            pltpu.VMEM((SIDE, LANES), jnp.float32),
            pltpu.VMEM(piece, jnp.float32),
            pltpu.VMEM((2 * faces, count, LANES), jnp.float32),
            pltpu.VMEM((4,) + cells, jnp.float32),
            pltpu.VMEM((3,) + cells, jnp.float32),
            pltpu.VMEM(piece, jnp.float32),
        ]
        + [dma] * 6
        + [dma((3,))],
        compiler_params=pltpu.CompilerParams(collective_id=0, has_side_effects=True),
    )(nbr_face.T, nbr_edge.T, state, jacobian, metric_diag, metric_cross, coriolis)
    return pl.pallas_call(
        last_kernel,
        out_shape=jax.ShapeDtypeStruct(state.shape, jnp.float32),
        in_specs=[vmem],
        out_specs=vmem,
        scratch_shapes=[pltpu.VMEM((faces, LANES, LANES), jnp.float32)],
    )(got)


def solution(mesh):
    groups, rows, columns = (mesh.shape[axis] for axis in ("face", "fy", "fx"))
    count = groups * rows * columns

    def body(*args):
        state = args[0]
        faces = state.shape[0]
        fits = rows == columns == 4 and 2 * count == HALF and faces * count <= LANES
        if fits and state.shape[1:] == (SIDE, SIDE, 3 * HALF) and 2 * faces <= SIDE:
            return by_level(groups, rows, *args)
        return per_device(*args)

    return jax.shard_map(
        body,
        mesh=mesh,
        in_specs=(
            P("face", "fy", "fx", None),
            P("face", "fy", "fx"),
            P(None, "face", "fy", "fx"),
            P("face", "fy", "fx"),
            P("face", "fy", "fx"),
            P(),
            P(),
        ),
        out_specs=P("face", "fy", "fx", None),
        check_vma=False,
    )
```

```python
import functools

import jax
import jax.numpy as jnp
import numpy as np
from jax import lax
from jax.experimental import pallas as pl
from jax.experimental.pallas import tpu as pltpu
from jax.sharding import PartitionSpec as P

time_step = 0.05
hyper_coeff = 0.0005
MESH = pl.DeviceIdType.MESH


def padded(cells, sides, width):
    for axis, dim in sides:
        count = lax.axis_size(axis)
        ends = count - 1
        head = lax.slice_in_dim(cells, 0, width, axis=dim)
        tail = lax.slice_in_dim(cells, cells.shape[dim] - width, cells.shape[dim], axis=dim)
        cells = jnp.concatenate(
            [
                lax.ppermute(tail, axis, [(i, (i + 1) % count) for i in range(ends)]),
                cells,
                lax.ppermute(head, axis, [((i + 1) % count, i) for i in range(ends)]),
            ],
            axis=dim,
        )
    return cells


def deriv_table():
    gll_nodes = np.array([-1.0, -1.0 / np.sqrt(5.0), 1.0 / np.sqrt(5.0), 1.0])
    bary_weights = np.ones(4)
    for j in range(4):
        for m in range(4):
            if m != j:
                bary_weights[j] = bary_weights[j] / (gll_nodes[j] - gll_nodes[m])
    matrix = np.zeros((4, 4))
    for i in range(4):
        for j in range(4):
            if i != j:
                matrix[i, j] = bary_weights[j] / bary_weights[i] / (gll_nodes[i] - gll_nodes[j])
        matrix[i, i] = -np.sum(matrix[i])
    return matrix


def along_x(values):
    face_count, row_count, col_count, chan_count = values.shape
    blocks = values.reshape(face_count, row_count, col_count // 4, 4, chan_count)
    result = jnp.einsum(
        "jk,abekc->abejc",
        jnp.asarray(deriv_table(), jnp.float32),
        blocks,
        precision=lax.Precision.HIGHEST,
    )
    return result.reshape(values.shape)


def along_y(values):
    face_count, row_count, col_count, chan_count = values.shape
    blocks = values.reshape(face_count, row_count // 4, 4, col_count, chan_count)
    result = jnp.einsum(
        "ik,aekxc->aeixc",
        jnp.asarray(deriv_table(), jnp.float32),
        blocks,
        precision=lax.Precision.HIGHEST,
    )
    return result.reshape(values.shape)


def mass_of(jacobian):
    weights = jnp.asarray([1.0 / 6.0, 5.0 / 6.0, 5.0 / 6.0, 1.0 / 6.0], jnp.float32)
    row_weight = jnp.tile(weights, jacobian.shape[1] // 4)
    col_weight = jnp.tile(weights, jacobian.shape[2] // 4)
    return jacobian * row_weight[None, :, None] * col_weight[None, None, :]


def tendency(state, geometry, planet):
    volume, metric_xx, metric_yy, metric_xy = geometry
    levels = state.shape[-1] // 3
    wind_u = state[..., :levels]
    wind_v = state[..., levels : 2 * levels]
    temper = state[..., 2 * levels :]
    contra_u = metric_xx * wind_u + metric_xy * wind_v
    contra_v = metric_xy * wind_u + metric_yy * wind_v
    energy = 0.5 * (wind_u * contra_u + wind_v * contra_v) + temper
    xderivs = along_x(jnp.concatenate([wind_v, temper, energy], -1))
    yderivs = along_y(jnp.concatenate([wind_u, temper, energy], -1))
    absolute = (xderivs[..., :levels] - yderivs[..., :levels]) / volume + planet
    tend_u = absolute * volume * contra_v - xderivs[..., 2 * levels :]
    tend_v = -absolute * volume * contra_u - yderivs[..., 2 * levels :]
    tend_t = -(
        contra_u * xderivs[..., levels : 2 * levels] + contra_v * yderivs[..., levels : 2 * levels]
    )
    return state + time_step * jnp.concatenate([tend_u, tend_v, tend_t], -1)


def laplace(values, geometry):
    volume, metric_xx, metric_yy, metric_xy = geometry
    grad_x = along_x(values)
    grad_y = along_y(values)
    flux_x = volume * (metric_xx * grad_x + metric_xy * grad_y)
    flux_y = volume * (metric_xy * grad_x + metric_yy * grad_y)
    return (along_x(flux_x) + along_y(flux_y)) / volume


def combine(values, axis):
    length = values.shape[axis] - 2
    positions = jnp.arange(length)
    leading = (positions % 4 == 0).astype(jnp.float32)
    trailing = (positions % 4 == 3).astype(jnp.float32)
    broad_shape = [1, 1, 1, 1]
    broad_shape[axis] = length
    leading = leading.reshape(broad_shape)
    trailing = trailing.reshape(broad_shape)
    middle = lax.slice_in_dim(values, 1, length + 1, axis=axis)
    previous = lax.slice_in_dim(values, 0, length, axis=axis)
    following = lax.slice_in_dim(values, 2, length + 2, axis=axis)
    return middle + leading * previous + trailing * following


def rotate(segment, quarter, levels):
    cosine = ((quarter == 0).astype(jnp.float32) - (quarter == 2).astype(jnp.float32))[..., None]
    sine_part = ((quarter == 1).astype(jnp.float32) - (quarter == 3).astype(jnp.float32))[..., None]
    wind_u = segment[..., :levels]
    wind_v = segment[..., levels : 2 * levels]
    return jnp.concatenate(
        [
            cosine * wind_u - sine_part * wind_v,
            sine_part * wind_u + cosine * wind_v,
            segment[..., 2 * levels :],
        ],
        -1,
    )


def in_face(values):
    across = combine(padded(values, (("fx", 2),), 1), 2)
    return combine(padded(across, (("fy", 1),), 1), 1)


def place_pieces(
    got_flat,
    got_tall,
    vector,
    nbr_edge,
    flat_edge,
    tall_edge,
    on_south,
    on_west,
    flat_start,
    tall_start,
    face_local,
    side_nodes,
    chan_count,
    levels,
):
    edge_ids = jnp.arange(4, dtype=jnp.int32)
    flat_target = nbr_edge[:, flat_edge]
    tall_target = nbr_edge[:, tall_edge]
    if vector:
        got_flat = rotate(got_flat, ((flat_target - flat_edge + 2) % 4)[None, :, None], levels)
        got_tall = rotate(got_tall, ((tall_target - tall_edge + 2) % 4)[None, :, None], levels)
    got_flat = jnp.where(on_south, got_flat[:, :, ::-1], got_flat)
    got_tall = jnp.where(on_west, got_tall, got_tall[:, :, ::-1])
    flat_pick = (flat_target[:, None] == edge_ids[None, :]).astype(jnp.float32)
    tall_pick = (tall_target[:, None] == edge_ids[None, :]).astype(jnp.float32)
    flat_rims = jnp.einsum("se,gsjc->gejc", flat_pick, got_flat, precision=lax.Precision.HIGHEST)
    tall_rims = jnp.einsum("se,gsjc->gejc", tall_pick, got_tall, precision=lax.Precision.HIGHEST)
    empty_rims = jnp.zeros((face_local, 4, side_nodes, chan_count), jnp.float32)
    rim_strips = lax.dynamic_update_slice(empty_rims, flat_rims, (0, 0, flat_start, 0))
    return rim_strips + lax.dynamic_update_slice(empty_rims, tall_rims, (0, 0, tall_start, 0))


def outgoing(
    summed, nbr_face, face_ids, flat_edge, tall_edge, on_south, on_west, flat_live, tall_live
):
    row_count = summed.shape[1]
    col_count = summed.shape[2]
    all_faces = jnp.arange(nbr_face.shape[0], dtype=jnp.int32)
    flat_piece = jnp.where(on_south, summed[:, 0], summed[:, row_count - 1])
    tall_piece = jnp.where(on_west, summed[:, :, 0], summed[:, :, col_count - 1])
    flat_dest = nbr_face[face_ids, flat_edge]
    tall_dest = nbr_face[face_ids, tall_edge]
    flat_send = ((all_faces[:, None] == flat_dest[None, :]) & flat_live).astype(jnp.float32)
    tall_send = ((all_faces[:, None] == tall_dest[None, :]) & tall_live).astype(jnp.float32)
    return (
        flat_send[:, :, None, None] * flat_piece[None],
        tall_send[:, :, None, None] * tall_piece[None],
    )


def assemble(values, vector, nbr_face, nbr_edge):
    summed = in_face(values)
    face_local, row_count, col_count, chan_count = summed.shape
    levels = chan_count // 3
    row_index = lax.axis_index("fy")
    col_index = lax.axis_index("fx")
    side_nodes = row_count * lax.axis_size("fy")
    face_ids = lax.axis_index("face") * face_local + jnp.arange(face_local, dtype=jnp.int32)
    on_south = row_index == 0
    on_north = row_index == lax.axis_size("fy") - 1
    on_west = col_index == 0
    on_east = col_index == lax.axis_size("fx") - 1
    flat_live = on_south | on_north
    tall_live = on_west | on_east
    flat_edge = jnp.where(on_south, 0, 2).astype(jnp.int32)
    tall_edge = jnp.where(on_west, 3, 1).astype(jnp.int32)
    flat_start = jnp.where(
        on_south, side_nodes - (col_index + 1) * col_count, col_index * col_count
    )
    tall_start = jnp.where(on_west, row_index * row_count, side_nodes - (row_index + 1) * row_count)
    send_flat, send_tall = outgoing(
        summed, nbr_face, face_ids, flat_edge, tall_edge, on_south, on_west, flat_live, tall_live
    )
    got_flat, got_tall = (
        lax.all_to_all(send_flat, "face", split_axis=0, concat_axis=1, tiled=True),
        lax.all_to_all(send_tall, "face", split_axis=0, concat_axis=1, tiled=True),
    )
    rim_strips = place_pieces(
        got_flat,
        got_tall,
        vector,
        nbr_edge,
        flat_edge,
        tall_edge,
        on_south,
        on_west,
        flat_start,
        tall_start,
        face_local,
        side_nodes,
        chan_count,
        levels,
    )
    flat_lines = jnp.stack([rim_strips[:, 0], rim_strips[:, 2, ::-1]], axis=1)
    flat_lines = flat_lines.reshape(face_local, 2, lax.axis_size("fx"), col_count, chan_count)
    tall_lines = jnp.stack([rim_strips[:, 1], rim_strips[:, 3, ::-1]], axis=1)
    tall_lines = tall_lines.reshape(face_local, 2, lax.axis_size("fy"), row_count, chan_count)
    flat_whole = lax.psum(flat_lines, "fy")
    tall_whole = lax.psum(tall_lines, "fx")
    flat_block = lax.psum_scatter(flat_whole, "fx", scatter_dimension=2, tiled=True)
    tall_block = lax.psum_scatter(tall_whole, "fy", scatter_dimension=2, tiled=True)
    flat_add = jnp.where(on_south, flat_block[:, 0, 0], flat_block[:, 1, 0])
    tall_add = jnp.where(on_west, tall_block[:, 1, 0], tall_block[:, 0, 0])
    result = summed.at[:, 0].add(jnp.where(on_south, flat_add, 0.0))
    result = result.at[:, row_count - 1].add(jnp.where(on_north, flat_add, 0.0))
    result = result.at[:, :, 0].add(jnp.where(on_west, tall_add, 0.0))
    result = result.at[:, :, col_count - 1].add(jnp.where(on_east, tall_add, 0.0))
    return result


def per_device(state, jacobian, metric_diag, metric_cross, coriolis, nbr_face, nbr_edge):
    node_mass = mass_of(jacobian)[..., None]
    total_mass = assemble(node_mass, False, nbr_face, nbr_edge)
    geometry = (
        jacobian[..., None],
        metric_diag[0][..., None],
        metric_diag[1][..., None],
        metric_cross[..., None],
    )
    raw = tendency(state, geometry, coriolis[..., None])
    sectioned = assemble(node_mass * raw, True, nbr_face, nbr_edge) / total_mass
    first_lap = (
        assemble(node_mass * laplace(sectioned, geometry), True, nbr_face, nbr_edge) / total_mass
    )
    second_lap = (
        assemble(node_mass * laplace(first_lap, geometry), True, nbr_face, nbr_edge) / total_mass
    )
    return sectioned - hyper_coeff * second_lap


SIDE = 8
HALF = 64
LANES = 128


def up(v, count, axis):
    return pltpu.roll(v, v.shape[axis] - count, axis)


def down(v, count, axis):
    return pltpu.roll(v, count, axis)


def slope(a):
    d = deriv_table()
    p0, p1, m0, m1 = a[0] + a[3], a[1] + a[2], a[0] - a[3], a[1] - a[2]
    bend = p0 - p1
    o0 = jnp.float32((d[0, 0] + d[0, 3]) / 2) * bend
    o1 = jnp.float32((d[1, 0] + d[1, 3]) / 2) * bend
    q0 = jnp.float32((d[0, 0] - d[0, 3]) / 2) * m0 + jnp.float32((d[0, 1] - d[0, 2]) / 2) * m1
    q1 = jnp.float32((d[1, 0] - d[1, 3]) / 2) * m0 + jnp.float32((d[1, 1] - d[1, 2]) / 2) * m1
    return [q0 + o0, q1 + o1, q1 - o1, q0 - o0]


def slope_x(v):
    return [slope(v[i]) for i in range(4)]


def slope_y(v):
    cols = [slope([v[i][j] for i in range(4)]) for j in range(4)]
    return [[cols[j][i] for j in range(4)] for i in range(4)]


def spread(mix, plane, er, i, which, v):
    for ec in range(2):
        mix[plane, pl.ds(er * 64 + ec * 32 + which * 16 + i * 4, 4), :] = v[4 * ec : 4 * ec + 4]


def by_node(mix, plane):
    return jnp.concatenate([mix[plane, pl.ds(n, 8, stride=16), :] for n in range(16)], axis=0)


def main_kernel(
    groups,
    blocks,
    nbr_face_in,
    nbr_edge_in,
    state_in,
    jac_in,
    diag_in,
    cross_in,
    coriolis_in,
    out,
    nbr_face,
    nbr_edge,
    state,
    jac,
    diag,
    cross,
    coriolis,
    mix,
    send,
    send_geo,
    got,
    got_geo,
    coef,
    section,
    back,
    sem_load,
    sem_s_geo,
    sem_r_geo,
    sem_s_in,
    sem_r_in,
    sem_s_out,
    sem_r_out,
    sem_own,
):
    faces = state.shape[0]
    count = groups * blocks * blocks
    last = blocks - 1
    g = lax.axis_index("face")
    y = lax.axis_index("fy")
    x = lax.axis_index("fx")
    me = (g * blocks + y) * blocks + x

    def by_distance(at):
        return [last - at, lax.rem(at + 2, 4), at + 1 - 2 * lax.rem(at, 2), at]

    def others(ys=(0, 1, 2, 3)):
        for k, tx in enumerate(by_distance(x)):
            for n in ys:
                ty = by_distance(y)[n]
                for dg in (1, 0):
                    if k < 3 or n < 3 or dg:
                        tg = lax.rem(g + dg, groups)
                        yield (tg * blocks + ty) * blocks + tx, (tg, ty, tx)

    loads = [
        pltpu.make_async_copy(src, dst, sem_load.at[n])
        for n, (src, dst) in enumerate(
            (
                (state_in, state),
                (jac_in, jac),
                (diag_in, diag),
                (cross_in, cross),
                (coriolis_in, coriolis),
                (nbr_face_in, nbr_face),
                (nbr_edge_in, nbr_edge),
            )
        )
    ]
    barrier = pltpu.get_barrier_semaphore()
    for _, at in others():
        pl.semaphore_signal(barrier, inc=1, device_id=at, device_id_type=MESH)
    for load in loads:
        load.start()
    for load in loads[1:]:
        load.wait()

    sub = lax.broadcasted_iota(jnp.int32, (SIDE, LANES), 0)
    lane = lax.broadcasted_iota(jnp.int32, (SIDE, LANES), 1)
    low = lane < HALF
    node = sub % 4
    table = deriv_table()
    weights = (1.0 / 6.0, 5.0 / 6.0, 5.0 / 6.0, 1.0 / 6.0)
    zero = jnp.zeros((SIDE, LANES), jnp.float32)

    def per_node(entries, at):
        total = jnp.full(at.shape, entries[0], jnp.float32)
        for n in range(1, 4):
            total = jnp.where(at == n, jnp.float32(entries[n]), total)
        return total

    taps = {
        s: per_node([float(table[n, n + s]) if 0 <= n + s < 4 else 0.0 for n in range(4)], node)
        for s in range(-3, 4)
    }

    def swap(v):
        return pltpu.roll(v, HALF, 1)

    def along_sub(v):
        total = taps[0] * v
        for s in (-3, -2, -1, 1, 2, 3):
            total = total + taps[s] * pltpu.roll(v, (-s) % SIDE, 0)
        return total

    def pick(v, at):
        return jnp.take_along_axis(v, at, axis=1, mode="promise_in_bounds")

    def spread_lanes(tiles):
        tiles = tiles + [tiles[0]] * (LANES // SIDE - len(tiles))
        return jnp.concatenate(tiles, axis=0).T

    tile_sub = lax.broadcasted_iota(jnp.int32, (SIDE, SIDE), 0) % 4
    tile_lane = lax.broadcasted_iota(jnp.int32, (SIDE, SIDE), 1) % 4
    tile_weight = per_node(weights, tile_sub) * per_node(weights, tile_lane)
    near_tiles, far_tiles = [], []
    for f in range(faces):
        vol, m_xx, m_yy, m_xy = jac[f], diag[0, f], diag[1, f], cross[f]
        mass = vol * tile_weight
        near_tiles += [m_xx, m_yy, m_xy, vol * coriolis[f], mass]
        far_tiles += [vol * m_xx, vol * m_yy, vol * m_xy, mass]
    local, shared = spread_lanes(near_tiles), spread_lanes(far_tiles)

    def spot(f, k, r):
        return (f * 5 + k) * SIDE + r

    cells = [(f, r) for f in range(faces) for r in range(SIDE)]
    lines = [[n + i for i in range(4)] for n in range(0, len(cells), 4)]
    for r in range(SIDE):
        for h in range(2):
            at = (lane // 2 % faces) * (4 * SIDE) + (2 * h + lane % 2) * SIDE + r
            spread(mix, faces, r // 4, r % 4, h, pick(shared, at))
    own = [pick(local, jnp.where(low, spot(f, 0, r), spot(f, 1, r))) for f, r in cells]
    skew = [pick(local, lane * 0 + spot(f, 2, r)) for f, r in cells]
    turn = [pick(local, lane * 0 + spot(f, 3, r)) for f, r in cells]
    mass = [pick(local, lane * 0 + spot(f, 4, r)) for f, r in cells]
    send_geo[...] = by_node(mix, faces).T[0:SIDE]
    loads[0].wait()
    wind = [state[f, r, :, 0 : 2 * HALF] for f, r in cells]
    temp = [state[f, r, :, 2 * HALF : 3 * HALF] for f, r in cells]
    temp = [jnp.concatenate([t, t], axis=1) for t in temp]
    other = [swap(w) for w in wind]
    contra = [m * w + n * o for m, n, w, o in zip(own, skew, wind, other)]
    power = [w * c for w, c in zip(wind, contra)]
    crossed = [swap(c) for c in contra]
    turned = [swap(p) for p in power]
    energy = [0.5 * (p + q) + t for p, q, t in zip(power, turned, temp)]

    def down_lines(v):
        out = [None] * len(cells)
        for line in lines:
            for n, d in zip(line, slope([v[n] for n in line])):
                out[n] = d
        return out

    dxs = [along_sub(jnp.where(low, e, w)) for e, w in zip(energy, wind)]
    dys = down_lines([jnp.where(low, w, e) for e, w in zip(energy, wind)])
    flow = [c * jnp.where(low, a, b) for c, a, b in zip(contra, [along_sub(t) for t in temp], down_lines(temp))]
    dxv = [swap(a) for a in dxs]
    dyu = [swap(a) for a in dys]
    flow = [q + swap(q) for q in flow]
    heat = [m * (t - time_step * q) for m, t, q in zip(mass, temp, flow)]
    fresh = []
    for n in range(len(cells)):
        spin = jnp.where(low, dxv[n] - dys[n], dyu[n] - dxs[n]) + jnp.where(low, turn[n], -turn[n])
        tend = spin * crossed[n] - jnp.where(low, dxs[n], dys[n])
        fresh.append(mass[n] * (wind[n] + time_step * tend))
    second = (lane >= 32) & (lane < 64)
    shifted = [(down(t, 32, 1), up(w, 32, 1)) for t, w in zip(heat, fresh)]
    for n, (f, r) in enumerate(cells):
        spread(mix, f, r // 4, r % 4, 0, jnp.where(second, shifted[n][0], fresh[n]))
        spread(mix, f, r // 4, r % 4, 1, jnp.where(second, heat[n], shifted[n][1]))
    for f in range(faces):
        turned = by_node(mix, f).T
        for k, part in enumerate((0, 2, 1)):
            send[k * faces + f] = turned[part * count : (part + 1) * count]

    er, ec, lev = sub // 4, (sub // 2) % 2, sub % 2
    lx, ly = lane % blocks, (lane // blocks) % blocks
    panel = lane // (blocks * blocks)
    er0, er1, ec0, ec1 = er == 0, er == 1, ec == 0, ec == 1
    x_lo, x_hi, y_lo, y_hi = lx == 0, lx == last, ly == 0, ly == last
    edge_at = (er0 & y_lo, er1 & x_hi, er0 & y_hi, er1 & x_lo)

    first_at = jnp.zeros((SIDE, LANES), jnp.int32)
    step_at, quarter_at = first_at, first_at
    for e in range(4):
        firsts, steps, quarters = first_at * 0, first_at * 0, first_at * 0
        for f in range(faces):
            for k in range(groups):
                nf = nbr_face[e, k * faces + f]
                ne = nbr_edge[e, k * faces + f]
                nl, ng = nf % faces, nf // faces
                tall = ne % 2
                step = 1 + tall * (blocks - 1)
                flips = jnp.where(ne >= 2, 0 if e < 2 else 1, 1 if e < 2 else 0)
                offset = jnp.where(ne == 2, last * blocks, jnp.where(ne == 1, last, 0))
                first = (nl * groups + ng) * (blocks * blocks) + offset + flips * (last * step)
                here = panel == f * groups + k
                firsts = jnp.where(here, first, firsts)
                steps = jnp.where(here, step * (1 - 2 * flips), steps)
                quarters = jnp.where(here, (e - ne + 2 + 4) % 4, quarters)
        first_at = jnp.where(edge_at[e], firsts, first_at)
        step_at = jnp.where(edge_at[e], steps, step_at)
        quarter_at = jnp.where(edge_at[e], quarters, quarter_at)
    source_at = first_at + step_at * jnp.where(er0, lx, ly)
    flipped = step_at < 0
    from_flat = (step_at == 1) | (step_at == -1)
    cosine = jnp.where(quarter_at == 0, 1.0, jnp.where(quarter_at == 2, -1.0, 0.0))
    sine = jnp.where(quarter_at == 1, 1.0, jnp.where(quarter_at == 3, -1.0, 0.0))

    def next_row(v):
        s = down(v, 4, 0)
        return jnp.where(er0, s, jnp.where(y_hi, zero, up(s, blocks, 1)))

    def prev_row(v):
        s = down(v, 4, 0)
        return jnp.where(er1, s, jnp.where(y_lo, zero, down(s, blocks, 1)))

    def next_col(v):
        return jnp.where(ec0, up(v, 2, 0), jnp.where(x_hi, zero, up(down(v, 2, 0), 1, 1)))

    def prev_col(v):
        return jnp.where(ec1, down(v, 2, 0), jnp.where(x_lo, zero, down(up(v, 2, 0), 1, 1)))

    def rims(v):
        found = []
        for b in range(4):
            flat = jnp.where(y_hi, v[3][b], v[0][b])
            flat = jnp.where(er0 == y_hi, down(flat, 4, 0), flat)
            tall = jnp.where(x_hi, v[b][3], v[b][0])
            tall = jnp.where(ec0 == x_hi, jnp.where(x_hi, up(tall, 2, 0), down(tall, 2, 0)), tall)
            tall = jnp.where(er == ec, tall, down(tall, 4, 0))
            found.append(jnp.where(from_flat, pick(flat, source_at), pick(tall, source_at)))
        partner = []
        for b in range(4):
            w = found[3 - b]
            w = jnp.where(ec0, up(w, 2, 0), down(w, 2, 0))
            partner.append(jnp.where(flipped, w, found[b]))
        return partner

    def glue(v, partner):
        v = [list(row) for row in v]
        sides = []
        for j in range(4):
            a, b, p = v[0][j], v[3][j], partner[j]
            s = down(p, 4, 0)
            v[0][j] = a + jnp.where(edge_at[0], p, prev_row(b))
            v[3][j] = b + jnp.where(er1 & y_hi, s, next_row(a))
            q = jnp.where(er1, p, s)
            q = jnp.where(er == ec, q, jnp.where(er0, down(q, 2, 0), up(q, 2, 0)))
            sides.append(q)
        q0, q3 = sides[0], sides[3]
        sides[0], sides[3] = q0 + prev_row(q3), q3 + next_row(q0)
        for i in range(4):
            a, b, q = v[i][0], v[i][3], sides[i]
            v[i][0] = a + jnp.where(ec0 & x_lo, q, prev_col(b))
            v[i][3] = b + jnp.where(ec1 & x_hi, q, next_col(a))
        return v

    def assemble_one(v):
        return glue(v, rims(v))

    def assemble_pair(u, v):
        pu, pv = rims(u), rims(v)
        tu = [cosine * a - sine * b for a, b in zip(pu, pv)]
        tv = [sine * a + cosine * b for a, b in zip(pu, pv)]
        return glue(u, tu), glue(v, tv)

    def grid(flat):
        return [[flat[8 * (4 * i + j) : 8 * (4 * i + j) + 8] for j in range(4)] for i in range(4)]

    def receive(ref, planes):
        blocks_in = [ref[p] for p in planes]
        blocks_in += [blocks_in[0]] * (LANES // count - len(blocks_in))
        return grid(jnp.concatenate(blocks_in, axis=0).T)

    def put(ref, k, v):
        for i in range(4):
            for j in range(4):
                ref[k, i, j] = v[i][j]

    def take(ref, k):
        return [[ref[k, i, j] for j in range(4)] for i in range(4)]

    def each(fn, *vs):
        return [[fn(*(v[i][j] for v in vs)) for j in range(4)] for i in range(4)]

    def copies(src_of, dst, sem_s, sem_r, ys=(0, 1, 2, 3)):
        for d, at in others(ys):
            pltpu.make_async_remote_copy(
                src_ref=src_of(d),
                dst_ref=dst,
                send_sem=sem_s,
                recv_sem=sem_r,
                device_id=at,
                device_id_type=MESH,
            ).start()

    def all_of(ref, sem_s, sem_r, first=0, planes=None, rows=None):
        planes = ref.shape[0] if planes is None else planes
        part = ref.at[pl.ds(first, planes), pl.ds(0, rows or count - 1)]
        return pltpu.make_async_remote_copy(
            src_ref=part,
            dst_ref=part,
            send_sem=sem_s,
            recv_sem=sem_r,
            device_id=(g, y, lax.rem(x + 1, blocks)),
            device_id_type=MESH,
        )

    pairs = 2 * faces
    half = count // 2
    parts = ((2 * faces, faces), (0, 2 * faces))
    pl.semaphore_wait(barrier, count - 1)
    odd = lax.rem(y, 2) == 1
    even = jnp.logical_not(odd)

    def send_shape(at):
        pltpu.make_async_remote_copy(
            src_ref=send_geo.at[pl.ds(0, pairs)],
            dst_ref=got_geo.at[:, me],
            send_sem=sem_s_geo.at[0],
            recv_sem=sem_r_geo.at[0],
            device_id=at,
            device_id_type=MESH,
        ).start()

    for k, tx in enumerate(by_distance(x)):
        for ty in (3 - y // 2 * 2, y // 2 * 2 + 1):
            for tg in (lax.rem(g + 1, groups), g):
                send_to = functools.partial(send_shape, (tg, ty, tx))
                if k == 3 and tg is g:
                    pl.when(jnp.logical_not((ty == y) & odd))(send_to)
                else:
                    send_to()
    for n, (first, planes) in enumerate(parts):
        part = pl.ds(first, planes)
        copies(lambda d: send.at[part, d], got.at[part, me], sem_s_in.at[n], sem_r_in.at[n])

    @pl.when(odd)
    def _():
        for q in range(pairs):
            got_geo[q, pl.ds(me, 1), :] = send_geo[pl.ds(q, 1), :]

    for q in range(3 * faces):
        got[q, pl.ds(me, 1), :] = send[q, pl.ds(me, 1), :]

    relay = pltpu.make_async_remote_copy(
        src_ref=got_geo,
        dst_ref=got_geo,
        send_sem=sem_s_geo.at[1],
        recv_sem=sem_r_geo.at[1],
        device_id=(g, y + 1 - 2 * lax.rem(y, 2), x),
        device_id_type=MESH,
    )

    def shapes(rows):
        return all_of(got_geo, sem_s_geo.at[0], sem_r_geo.at[0], rows=rows)

    @pl.when(odd)
    def _():
        shapes(count - 1).wait_recv()
        relay.start()

    pl.when(even)(relay.wait_recv)
    for p in range(2):
        both = receive(got_geo, range(p, pairs, 2))
        put(coef, 2 * p, each(lambda v: jnp.where(lev == 0, v, down(v, 1, 0)), both))
        put(coef, 2 * p + 1, each(lambda v: jnp.where(lev == 1, v, up(v, 1, 0)), both))
    put(coef, 3, each(lambda v: 1.0 / v, assemble_one(take(coef, 3))))

    def fields_in(k):
        return receive(got, range(k * faces, (k + 1) * faces))

    def scaled(v):
        return each(lambda a, b: a * b, v, take(coef, 3))

    def laplace_of(v):
        a, b, c = take(coef, 0), take(coef, 1), take(coef, 2)
        gx, gy = slope_x(v), slope_y(v)
        fx = each(lambda p, q, m, n: m * p + n * q, gx, gy, a, b)
        fy = each(lambda p, q, m, n: m * p + n * q, gx, gy, b, c)
        total = each(lambda p, q: p + q, slope_x(fx), slope_y(fy))
        return [[jnp.float32(weights[i] * weights[j]) * total[i][j] for j in range(4)] for i in range(4)]

    def finish(k, v):
        done = each(lambda s, a: s - hyper_coeff * a, take(section, k), v)
        turned = jnp.concatenate([done[i][j] for i in range(4) for j in range(4)], axis=0).T
        for f in range(faces):
            back[k * faces + f] = turned[f * count : (f + 1) * count]

    def send_back(k, n):
        part = pl.ds(k * faces, n * faces)
        copies(lambda d: back.at[part, d], out.at[part, me], sem_s_out, sem_r_out)
        own = pltpu.make_async_copy(back.at[part, me], out.at[part, me], sem_own.at[k])
        own.start()
        return own

    def arrived(n):
        first, planes = parts[n]
        return all_of(got, sem_s_in.at[n], sem_r_in.at[n], first, planes)

    arrived(0).wait_recv()
    heat = scaled(assemble_one(fields_in(2)))
    put(section, 2, heat)
    heat = scaled(assemble_one(laplace_of(heat)))
    heat = scaled(assemble_one(laplace_of(heat)))
    finish(2, heat)
    own_t = send_back(2, 1)
    arrived(1).wait_recv()
    wind_u, wind_v = assemble_pair(fields_in(0), fields_in(1))
    put(section, 0, scaled(wind_u))
    put(section, 1, scaled(wind_v))
    wind_u, wind_v = assemble_pair(laplace_of(take(section, 0)), laplace_of(take(section, 1)))
    wind_u, wind_v = assemble_pair(laplace_of(scaled(wind_u)), laplace_of(scaled(wind_v)))
    finish(0, scaled(wind_u))
    finish(1, scaled(wind_v))
    own_w = send_back(0, 2)

    @pl.when(odd)
    def _():
        shapes(half - 1).wait_send()
        relay.wait_send()

    pl.when(even)(shapes(half).wait_send)
    arrived(0).wait_send()
    arrived(1).wait_send()
    own_t.wait()
    own_w.wait()
    all_of(out, sem_s_out, sem_r_out).wait_send()
    all_of(out, sem_s_out, sem_r_out).wait_recv()


def last_kernel(got, out, mix):
    faces = out.shape[0]
    lane = lax.broadcasted_iota(jnp.int32, (SIDE, LANES), 1)
    even = (lane // 32) % 2 == 0
    for f in range(faces):
        u, v, t = (got[k * faces + f] for k in range(3))
        turned = jnp.concatenate([u, t, v, v], axis=0).T
        for n in range(16):
            mix[f, pl.ds(n, 8, stride=16), :] = turned[8 * n : 8 * n + 8]
        for r in range(SIDE):
            start = (r // 4) * 64 + (r % 4) * 4
            a, b = (
                jnp.concatenate([mix[f, pl.ds(start + h * 16 + ec * 32, 4), :] for ec in range(2)], axis=0)
                for h in range(2)
            )
            out[f, r, :, 0 : 2 * HALF] = jnp.where(even, a, down(b, 32, 1))
            out[f, r, :, 2 * HALF : 3 * HALF] = jnp.where(even, up(a, 32, 1), b)[:, 0:HALF]


def by_level(groups, blocks, state, jacobian, metric_diag, metric_cross, coriolis, nbr_face, nbr_edge):
    faces = state.shape[0]
    count = groups * blocks * blocks
    vmem, anywhere = pl.BlockSpec(memory_space=pltpu.VMEM), pl.BlockSpec(memory_space=pl.ANY)
    inputs = (nbr_face.T, nbr_edge.T, state, jacobian, metric_diag, metric_cross, coriolis)
    inputs = [pltpu.with_memory_space_constraint(a, pltpu.HBM) for a in inputs]
    piece = (3 * faces, count, LANES)
    cells = (4, 4, SIDE, LANES)
    dma = pltpu.SemaphoreType.DMA
    got = pl.pallas_call(
        functools.partial(main_kernel, groups, blocks),
        out_shape=jax.ShapeDtypeStruct(piece, jnp.float32),
        in_specs=[pl.BlockSpec(memory_space=pltpu.HBM)] * 7,
        out_specs=anywhere,
        scratch_shapes=[pltpu.SMEM(a.shape, a.dtype) for a in inputs[:2]]
        + [pltpu.VMEM(a.shape, a.dtype) for a in inputs[2:]]
        + [
            pltpu.VMEM((faces + 1, LANES, LANES), jnp.float32),
            pltpu.VMEM(piece, jnp.float32),
            pltpu.VMEM((SIDE, LANES), jnp.float32),
            pltpu.VMEM(piece, jnp.float32),
            pltpu.VMEM((2 * faces, count, LANES), jnp.float32),
            pltpu.VMEM((4,) + cells, jnp.float32),
            pltpu.VMEM((3,) + cells, jnp.float32),
            pltpu.VMEM(piece, jnp.float32),
        ]
        + [dma((7,)), dma((2,)), dma((2,)), dma((2,)), dma((2,)), dma, dma, dma((3,))],
        compiler_params=pltpu.CompilerParams(collective_id=0, has_side_effects=True, vmem_limit_bytes=16 << 20),
    )(*inputs)
    return pl.pallas_call(
        last_kernel,
        out_shape=jax.ShapeDtypeStruct(state.shape, jnp.float32),
        in_specs=[vmem],
        out_specs=vmem,
        scratch_shapes=[pltpu.VMEM((faces, LANES, LANES), jnp.float32)],
        compiler_params=pltpu.CompilerParams(vmem_limit_bytes=16 << 20),
    )(got)


def solution(mesh):
    groups, rows, columns = (mesh.shape[axis] for axis in ("face", "fy", "fx"))
    count = groups * rows * columns

    def body(*args):
        state = args[0]
        faces = state.shape[0]
        fits = rows == columns == 4 and 2 * count == HALF and faces * count <= LANES
        if fits and state.shape[1:] == (SIDE, SIDE, 3 * HALF) and 2 * faces <= SIDE:
            return by_level(groups, rows, *args)
        return per_device(*args)

    return jax.shard_map(
        body,
        mesh=mesh,
        in_specs=(
            P("face", "fy", "fx", None),
            P("face", "fy", "fx"),
            P(None, "face", "fy", "fx"),
            P("face", "fy", "fx"),
            P("face", "fy", "fx"),
            P(),
            P(),
        ),
        out_specs=P("face", "fy", "fx", None),
        check_vma=False,
    )
```

```python
import functools

import jax
import jax.numpy as jnp
import numpy as np
from jax import lax
from jax.experimental import pallas as pl
from jax.experimental.pallas import tpu as pltpu
from jax.sharding import PartitionSpec as P

time_step = 0.05
hyper_coeff = 0.0005
MESH = pl.DeviceIdType.MESH


def padded(cells, sides, width):
    for axis, dim in sides:
        count = lax.axis_size(axis)
        ends = count - 1
        head = lax.slice_in_dim(cells, 0, width, axis=dim)
        tail = lax.slice_in_dim(cells, cells.shape[dim] - width, cells.shape[dim], axis=dim)
        cells = jnp.concatenate(
            [
                lax.ppermute(tail, axis, [(i, (i + 1) % count) for i in range(ends)]),
                cells,
                lax.ppermute(head, axis, [((i + 1) % count, i) for i in range(ends)]),
            ],
            axis=dim,
        )
    return cells


def deriv_table():
    gll_nodes = np.array([-1.0, -1.0 / np.sqrt(5.0), 1.0 / np.sqrt(5.0), 1.0])
    bary_weights = np.ones(4)
    for j in range(4):
        for m in range(4):
            if m != j:
                bary_weights[j] = bary_weights[j] / (gll_nodes[j] - gll_nodes[m])
    matrix = np.zeros((4, 4))
    for i in range(4):
        for j in range(4):
            if i != j:
                matrix[i, j] = bary_weights[j] / bary_weights[i] / (gll_nodes[i] - gll_nodes[j])
        matrix[i, i] = -np.sum(matrix[i])
    return matrix


def along_x(values):
    face_count, row_count, col_count, chan_count = values.shape
    blocks = values.reshape(face_count, row_count, col_count // 4, 4, chan_count)
    result = jnp.einsum(
        "jk,abekc->abejc",
        jnp.asarray(deriv_table(), jnp.float32),
        blocks,
        precision=lax.Precision.HIGHEST,
    )
    return result.reshape(values.shape)


def along_y(values):
    face_count, row_count, col_count, chan_count = values.shape
    blocks = values.reshape(face_count, row_count // 4, 4, col_count, chan_count)
    result = jnp.einsum(
        "ik,aekxc->aeixc",
        jnp.asarray(deriv_table(), jnp.float32),
        blocks,
        precision=lax.Precision.HIGHEST,
    )
    return result.reshape(values.shape)


def mass_of(jacobian):
    weights = jnp.asarray([1.0 / 6.0, 5.0 / 6.0, 5.0 / 6.0, 1.0 / 6.0], jnp.float32)
    row_weight = jnp.tile(weights, jacobian.shape[1] // 4)
    col_weight = jnp.tile(weights, jacobian.shape[2] // 4)
    return jacobian * row_weight[None, :, None] * col_weight[None, None, :]


def tendency(state, geometry, planet):
    volume, metric_xx, metric_yy, metric_xy = geometry
    levels = state.shape[-1] // 3
    wind_u = state[..., :levels]
    wind_v = state[..., levels : 2 * levels]
    temper = state[..., 2 * levels :]
    contra_u = metric_xx * wind_u + metric_xy * wind_v
    contra_v = metric_xy * wind_u + metric_yy * wind_v
    energy = 0.5 * (wind_u * contra_u + wind_v * contra_v) + temper
    xderivs = along_x(jnp.concatenate([wind_v, temper, energy], -1))
    yderivs = along_y(jnp.concatenate([wind_u, temper, energy], -1))
    absolute = (xderivs[..., :levels] - yderivs[..., :levels]) / volume + planet
    tend_u = absolute * volume * contra_v - xderivs[..., 2 * levels :]
    tend_v = -absolute * volume * contra_u - yderivs[..., 2 * levels :]
    tend_t = -(
        contra_u * xderivs[..., levels : 2 * levels] + contra_v * yderivs[..., levels : 2 * levels]
    )
    return state + time_step * jnp.concatenate([tend_u, tend_v, tend_t], -1)


def laplace(values, geometry):
    volume, metric_xx, metric_yy, metric_xy = geometry
    grad_x = along_x(values)
    grad_y = along_y(values)
    flux_x = volume * (metric_xx * grad_x + metric_xy * grad_y)
    flux_y = volume * (metric_xy * grad_x + metric_yy * grad_y)
    return (along_x(flux_x) + along_y(flux_y)) / volume


def combine(values, axis):
    length = values.shape[axis] - 2
    positions = jnp.arange(length)
    leading = (positions % 4 == 0).astype(jnp.float32)
    trailing = (positions % 4 == 3).astype(jnp.float32)
    broad_shape = [1, 1, 1, 1]
    broad_shape[axis] = length
    leading = leading.reshape(broad_shape)
    trailing = trailing.reshape(broad_shape)
    middle = lax.slice_in_dim(values, 1, length + 1, axis=axis)
    previous = lax.slice_in_dim(values, 0, length, axis=axis)
    following = lax.slice_in_dim(values, 2, length + 2, axis=axis)
    return middle + leading * previous + trailing * following


def rotate(segment, quarter, levels):
    cosine = ((quarter == 0).astype(jnp.float32) - (quarter == 2).astype(jnp.float32))[..., None]
    sine_part = ((quarter == 1).astype(jnp.float32) - (quarter == 3).astype(jnp.float32))[..., None]
    wind_u = segment[..., :levels]
    wind_v = segment[..., levels : 2 * levels]
    return jnp.concatenate(
        [
            cosine * wind_u - sine_part * wind_v,
            sine_part * wind_u + cosine * wind_v,
            segment[..., 2 * levels :],
        ],
        -1,
    )


def in_face(values):
    across = combine(padded(values, (("fx", 2),), 1), 2)
    return combine(padded(across, (("fy", 1),), 1), 1)


def place_pieces(
    got_flat,
    got_tall,
    vector,
    nbr_edge,
    flat_edge,
    tall_edge,
    on_south,
    on_west,
    flat_start,
    tall_start,
    face_local,
    side_nodes,
    chan_count,
    levels,
):
    edge_ids = jnp.arange(4, dtype=jnp.int32)
    flat_target = nbr_edge[:, flat_edge]
    tall_target = nbr_edge[:, tall_edge]
    if vector:
        got_flat = rotate(got_flat, ((flat_target - flat_edge + 2) % 4)[None, :, None], levels)
        got_tall = rotate(got_tall, ((tall_target - tall_edge + 2) % 4)[None, :, None], levels)
    got_flat = jnp.where(on_south, got_flat[:, :, ::-1], got_flat)
    got_tall = jnp.where(on_west, got_tall, got_tall[:, :, ::-1])
    flat_pick = (flat_target[:, None] == edge_ids[None, :]).astype(jnp.float32)
    tall_pick = (tall_target[:, None] == edge_ids[None, :]).astype(jnp.float32)
    flat_rims = jnp.einsum("se,gsjc->gejc", flat_pick, got_flat, precision=lax.Precision.HIGHEST)
    tall_rims = jnp.einsum("se,gsjc->gejc", tall_pick, got_tall, precision=lax.Precision.HIGHEST)
    empty_rims = jnp.zeros((face_local, 4, side_nodes, chan_count), jnp.float32)
    rim_strips = lax.dynamic_update_slice(empty_rims, flat_rims, (0, 0, flat_start, 0))
    return rim_strips + lax.dynamic_update_slice(empty_rims, tall_rims, (0, 0, tall_start, 0))


def outgoing(
    summed, nbr_face, face_ids, flat_edge, tall_edge, on_south, on_west, flat_live, tall_live
):
    row_count = summed.shape[1]
    col_count = summed.shape[2]
    all_faces = jnp.arange(nbr_face.shape[0], dtype=jnp.int32)
    flat_piece = jnp.where(on_south, summed[:, 0], summed[:, row_count - 1])
    tall_piece = jnp.where(on_west, summed[:, :, 0], summed[:, :, col_count - 1])
    flat_dest = nbr_face[face_ids, flat_edge]
    tall_dest = nbr_face[face_ids, tall_edge]
    flat_send = ((all_faces[:, None] == flat_dest[None, :]) & flat_live).astype(jnp.float32)
    tall_send = ((all_faces[:, None] == tall_dest[None, :]) & tall_live).astype(jnp.float32)
    return (
        flat_send[:, :, None, None] * flat_piece[None],
        tall_send[:, :, None, None] * tall_piece[None],
    )


def assemble(values, vector, nbr_face, nbr_edge):
    summed = in_face(values)
    face_local, row_count, col_count, chan_count = summed.shape
    levels = chan_count // 3
    row_index = lax.axis_index("fy")
    col_index = lax.axis_index("fx")
    side_nodes = row_count * lax.axis_size("fy")
    face_ids = lax.axis_index("face") * face_local + jnp.arange(face_local, dtype=jnp.int32)
    on_south = row_index == 0
    on_north = row_index == lax.axis_size("fy") - 1
    on_west = col_index == 0
    on_east = col_index == lax.axis_size("fx") - 1
    flat_live = on_south | on_north
    tall_live = on_west | on_east
    flat_edge = jnp.where(on_south, 0, 2).astype(jnp.int32)
    tall_edge = jnp.where(on_west, 3, 1).astype(jnp.int32)
    flat_start = jnp.where(
        on_south, side_nodes - (col_index + 1) * col_count, col_index * col_count
    )
    tall_start = jnp.where(on_west, row_index * row_count, side_nodes - (row_index + 1) * row_count)
    send_flat, send_tall = outgoing(
        summed, nbr_face, face_ids, flat_edge, tall_edge, on_south, on_west, flat_live, tall_live
    )
    got_flat, got_tall = (
        lax.all_to_all(send_flat, "face", split_axis=0, concat_axis=1, tiled=True),
        lax.all_to_all(send_tall, "face", split_axis=0, concat_axis=1, tiled=True),
    )
    rim_strips = place_pieces(
        got_flat,
        got_tall,
        vector,
        nbr_edge,
        flat_edge,
        tall_edge,
        on_south,
        on_west,
        flat_start,
        tall_start,
        face_local,
        side_nodes,
        chan_count,
        levels,
    )
    flat_lines = jnp.stack([rim_strips[:, 0], rim_strips[:, 2, ::-1]], axis=1)
    flat_lines = flat_lines.reshape(face_local, 2, lax.axis_size("fx"), col_count, chan_count)
    tall_lines = jnp.stack([rim_strips[:, 1], rim_strips[:, 3, ::-1]], axis=1)
    tall_lines = tall_lines.reshape(face_local, 2, lax.axis_size("fy"), row_count, chan_count)
    flat_whole = lax.psum(flat_lines, "fy")
    tall_whole = lax.psum(tall_lines, "fx")
    flat_block = lax.psum_scatter(flat_whole, "fx", scatter_dimension=2, tiled=True)
    tall_block = lax.psum_scatter(tall_whole, "fy", scatter_dimension=2, tiled=True)
    flat_add = jnp.where(on_south, flat_block[:, 0, 0], flat_block[:, 1, 0])
    tall_add = jnp.where(on_west, tall_block[:, 1, 0], tall_block[:, 0, 0])
    result = summed.at[:, 0].add(jnp.where(on_south, flat_add, 0.0))
    result = result.at[:, row_count - 1].add(jnp.where(on_north, flat_add, 0.0))
    result = result.at[:, :, 0].add(jnp.where(on_west, tall_add, 0.0))
    result = result.at[:, :, col_count - 1].add(jnp.where(on_east, tall_add, 0.0))
    return result


def per_device(state, jacobian, metric_diag, metric_cross, coriolis, nbr_face, nbr_edge):
    node_mass = mass_of(jacobian)[..., None]
    total_mass = assemble(node_mass, False, nbr_face, nbr_edge)
    geometry = (
        jacobian[..., None],
        metric_diag[0][..., None],
        metric_diag[1][..., None],
        metric_cross[..., None],
    )
    raw = tendency(state, geometry, coriolis[..., None])
    sectioned = assemble(node_mass * raw, True, nbr_face, nbr_edge) / total_mass
    first_lap = (
        assemble(node_mass * laplace(sectioned, geometry), True, nbr_face, nbr_edge) / total_mass
    )
    second_lap = (
        assemble(node_mass * laplace(first_lap, geometry), True, nbr_face, nbr_edge) / total_mass
    )
    return sectioned - hyper_coeff * second_lap


SIDE = 8
HALF = 64
LANES = 128


IN_KINDS = "gggtttwwwgtw"
IN_COLUMNS = ("321321321000", "320320320111", "301301301222", "012012012333")


def up(v, count, axis):
    return pltpu.roll(v, v.shape[axis] - count, axis)


def down(v, count, axis):
    return pltpu.roll(v, count, axis)


def slope(a):
    d = deriv_table()
    p0, p1, m0, m1 = a[0] + a[3], a[1] + a[2], a[0] - a[3], a[1] - a[2]
    bend = p0 - p1
    o0 = jnp.float32((d[0, 0] + d[0, 3]) / 2) * bend
    o1 = jnp.float32((d[1, 0] + d[1, 3]) / 2) * bend
    q0 = jnp.float32((d[0, 0] - d[0, 3]) / 2) * m0 + jnp.float32((d[0, 1] - d[0, 2]) / 2) * m1
    q1 = jnp.float32((d[1, 0] - d[1, 3]) / 2) * m0 + jnp.float32((d[1, 1] - d[1, 2]) / 2) * m1
    return [q0 + o0, q1 + o1, q1 - o1, q0 - o0]


def slope_x(v):
    return [slope(v[i]) for i in range(4)]


def slope_y(v):
    cols = [slope([v[i][j] for i in range(4)]) for j in range(4)]
    return [[cols[j][i] for j in range(4)] for i in range(4)]


def spread(mix, plane, er, i, which, v):
    for ec in range(2):
        mix[plane, pl.ds(er * 64 + ec * 32 + which * 16 + i * 4, 4), :] = v[4 * ec : 4 * ec + 4]


def by_node(mix, plane):
    return jnp.concatenate([mix[plane, pl.ds(n, 8, stride=16), :] for n in range(16)], axis=0)


def main_kernel(
    groups,
    blocks,
    nbr_face_in,
    nbr_edge_in,
    state_in,
    jac_in,
    diag_in,
    cross_in,
    coriolis_in,
    out,
    nbr_face,
    nbr_edge,
    state,
    jac,
    diag,
    cross,
    coriolis,
    mix,
    send,
    send_geo,
    got,
    got_geo,
    coef,
    section,
    back,
    sem_load,
    sem_s_geo,
    sem_r_geo,
    sem_s_in,
    sem_r_in,
    sem_s_out,
    sem_r_out,
    sem_own,
):
    faces = state.shape[0]
    count = groups * blocks * blocks
    last = blocks - 1
    g = lax.axis_index("face")
    y = lax.axis_index("fy")
    x = lax.axis_index("fx")
    me = (g * blocks + y) * blocks + x

    def by_distance(at):
        return [last - at, lax.rem(at + 2, 4), at + 1 - 2 * lax.rem(at, 2), at]

    def others(columns):
        for n, tx in enumerate(columns):
            for ty in by_distance(y)[: blocks - 1] + [y]:
                for tg in (lax.rem(g + 1, groups), g):
                    if tx is not x or ty is not y or tg is not g:
                        yield (tg * blocks + ty) * blocks + tx, (tg, ty, tx)

    def towards(columns):
        for tx in columns:
            for ty in range(blocks):
                for tg in range(groups):
                    yield (tg * blocks + ty) * blocks + tx, (tg, ty, tx)

    loads = [
        pltpu.make_async_copy(src, dst, sem_load.at[n])
        for n, (src, dst) in enumerate(
            (
                (state_in, state),
                (jac_in, jac),
                (diag_in, diag),
                (cross_in, cross),
                (coriolis_in, coriolis),
                (nbr_face_in, nbr_face),
                (nbr_edge_in, nbr_edge),
            )
        )
    ]
    barrier = pltpu.get_barrier_semaphore()
    for _, at in others(by_distance(x)):
        pl.semaphore_signal(barrier, inc=1, device_id=at, device_id_type=MESH)
    for load in loads:
        load.start()
    for load in loads[1:]:
        load.wait()

    sub = lax.broadcasted_iota(jnp.int32, (SIDE, LANES), 0)
    lane = lax.broadcasted_iota(jnp.int32, (SIDE, LANES), 1)
    low = lane < HALF
    node = sub % 4
    table = deriv_table()
    weights = (1.0 / 6.0, 5.0 / 6.0, 5.0 / 6.0, 1.0 / 6.0)
    zero = jnp.zeros((SIDE, LANES), jnp.float32)

    def per_node(entries, at):
        total = jnp.full(at.shape, entries[0], jnp.float32)
        for n in range(1, 4):
            total = jnp.where(at == n, jnp.float32(entries[n]), total)
        return total

    taps = {
        s: per_node([float(table[n, n + s]) if 0 <= n + s < 4 else 0.0 for n in range(4)], node)
        for s in range(-3, 4)
    }

    def swap(v):
        return pltpu.roll(v, HALF, 1)

    def along_sub(v):
        total = taps[0] * v
        for s in (-3, -2, -1, 1, 2, 3):
            total = total + taps[s] * pltpu.roll(v, (-s) % SIDE, 0)
        return total

    def pick(v, at):
        return jnp.take_along_axis(v, at, axis=1, mode="promise_in_bounds")

    def spread_lanes(tiles):
        tiles = tiles + [tiles[0]] * (LANES // SIDE - len(tiles))
        return jnp.concatenate(tiles, axis=0).T

    tile_sub = lax.broadcasted_iota(jnp.int32, (SIDE, SIDE), 0) % 4
    tile_lane = lax.broadcasted_iota(jnp.int32, (SIDE, SIDE), 1) % 4
    tile_weight = per_node(weights, tile_sub) * per_node(weights, tile_lane)
    near_tiles, far_tiles = [], []
    for f in range(faces):
        vol, m_xx, m_yy, m_xy = jac[f], diag[0, f], diag[1, f], cross[f]
        mass = vol * tile_weight
        near_tiles += [m_xx, m_yy, m_xy, vol * coriolis[f], mass]
        far_tiles += [vol * m_xx, vol * m_yy, vol * m_xy, mass]
    local, shared = spread_lanes(near_tiles), spread_lanes(far_tiles)

    def spot(f, k, r):
        return (f * 5 + k) * SIDE + r

    cells = [(f, r) for f in range(faces) for r in range(SIDE)]
    lines = [[n + i for i in range(4)] for n in range(0, len(cells), 4)]
    for r in range(SIDE):
        for h in range(2):
            at = (lane // 2 % faces) * (4 * SIDE) + (2 * h + lane % 2) * SIDE + r
            spread(mix, faces, r // 4, r % 4, h, pick(shared, at))
    own = [pick(local, jnp.where(low, spot(f, 0, r), spot(f, 1, r))) for f, r in cells]
    skew = [pick(local, lane * 0 + spot(f, 2, r)) for f, r in cells]
    turn = [pick(local, lane * 0 + spot(f, 3, r)) for f, r in cells]
    mass = [pick(local, lane * 0 + spot(f, 4, r)) for f, r in cells]
    send_geo[...] = by_node(mix, faces).T[0:SIDE]
    loads[0].wait()
    wind = [state[f, r, :, 0 : 2 * HALF] for f, r in cells]
    temp = [state[f, r, :, 2 * HALF : 3 * HALF] for f, r in cells]
    temp = [jnp.concatenate([t, t], axis=1) for t in temp]
    other = [swap(w) for w in wind]
    contra = [m * w + n * o for m, n, w, o in zip(own, skew, wind, other)]
    power = [w * c for w, c in zip(wind, contra)]
    crossed = [swap(c) for c in contra]
    turned = [swap(p) for p in power]
    energy = [0.5 * (p + q) + t for p, q, t in zip(power, turned, temp)]

    def down_lines(v):
        out = [None] * len(cells)
        for line in lines:
            for n, d in zip(line, slope([v[n] for n in line])):
                out[n] = d
        return out

    dxs = [along_sub(jnp.where(low, e, w)) for e, w in zip(energy, wind)]
    dys = down_lines([jnp.where(low, w, e) for e, w in zip(energy, wind)])
    flow = [c * jnp.where(low, a, b) for c, a, b in zip(contra, [along_sub(t) for t in temp], down_lines(temp))]
    dxv = [swap(a) for a in dxs]
    dyu = [swap(a) for a in dys]
    flow = [q + swap(q) for q in flow]
    heat = [m * (t - time_step * q) for m, t, q in zip(mass, temp, flow)]
    fresh = []
    for n in range(len(cells)):
        spin = jnp.where(low, dxv[n] - dys[n], dyu[n] - dxs[n]) + jnp.where(low, turn[n], -turn[n])
        tend = spin * crossed[n] - jnp.where(low, dxs[n], dys[n])
        fresh.append(mass[n] * (wind[n] + time_step * tend))
    second = (lane >= 32) & (lane < 64)
    shifted = [(down(t, 32, 1), up(w, 32, 1)) for t, w in zip(heat, fresh)]
    for n, (f, r) in enumerate(cells):
        spread(mix, f, r // 4, r % 4, 0, jnp.where(second, shifted[n][0], fresh[n]))
        spread(mix, f, r // 4, r % 4, 1, jnp.where(second, heat[n], shifted[n][1]))
    for f in range(faces):
        turned = by_node(mix, f).T
        for k, part in enumerate((0, 2, 1)):
            send[k * faces + f] = turned[part * count : (part + 1) * count]

    er, ec, lev = sub // 4, (sub // 2) % 2, sub % 2
    lx, ly = lane % blocks, (lane // blocks) % blocks
    panel = lane // (blocks * blocks)
    er0, er1, ec0, ec1 = er == 0, er == 1, ec == 0, ec == 1
    x_lo, x_hi, y_lo, y_hi = lx == 0, lx == last, ly == 0, ly == last
    edge_at = (er0 & y_lo, er1 & x_hi, er0 & y_hi, er1 & x_lo)

    first_at = jnp.zeros((SIDE, LANES), jnp.int32)
    step_at, quarter_at = first_at, first_at
    for e in range(4):
        firsts, steps, quarters = first_at * 0, first_at * 0, first_at * 0
        for f in range(faces):
            for k in range(groups):
                nf = nbr_face[e, k * faces + f]
                ne = nbr_edge[e, k * faces + f]
                nl, ng = nf % faces, nf // faces
                tall = ne % 2
                step = 1 + tall * (blocks - 1)
                flips = jnp.where(ne >= 2, 0 if e < 2 else 1, 1 if e < 2 else 0)
                offset = jnp.where(ne == 2, last * blocks, jnp.where(ne == 1, last, 0))
                first = (nl * groups + ng) * (blocks * blocks) + offset + flips * (last * step)
                here = panel == f * groups + k
                firsts = jnp.where(here, first, firsts)
                steps = jnp.where(here, step * (1 - 2 * flips), steps)
                quarters = jnp.where(here, (e - ne + 2 + 4) % 4, quarters)
        first_at = jnp.where(edge_at[e], firsts, first_at)
        step_at = jnp.where(edge_at[e], steps, step_at)
        quarter_at = jnp.where(edge_at[e], quarters, quarter_at)
    source_at = first_at + step_at * jnp.where(er0, lx, ly)
    flipped = step_at < 0
    from_flat = (step_at == 1) | (step_at == -1)
    cosine = jnp.where(quarter_at == 0, 1.0, jnp.where(quarter_at == 2, -1.0, 0.0))
    sine = jnp.where(quarter_at == 1, 1.0, jnp.where(quarter_at == 3, -1.0, 0.0))

    def next_row(v):
        s = down(v, 4, 0)
        return jnp.where(er0, s, jnp.where(y_hi, zero, up(s, blocks, 1)))

    def prev_row(v):
        s = down(v, 4, 0)
        return jnp.where(er1, s, jnp.where(y_lo, zero, down(s, blocks, 1)))

    def next_col(v):
        return jnp.where(ec0, up(v, 2, 0), jnp.where(x_hi, zero, up(down(v, 2, 0), 1, 1)))

    def prev_col(v):
        return jnp.where(ec1, down(v, 2, 0), jnp.where(x_lo, zero, down(up(v, 2, 0), 1, 1)))

    def rims(v):
        found = []
        for b in range(4):
            flat = jnp.where(y_hi, v[3][b], v[0][b])
            flat = jnp.where(er0 == y_hi, down(flat, 4, 0), flat)
            tall = jnp.where(x_hi, v[b][3], v[b][0])
            tall = jnp.where(ec0 == x_hi, jnp.where(x_hi, up(tall, 2, 0), down(tall, 2, 0)), tall)
            tall = jnp.where(er == ec, tall, down(tall, 4, 0))
            found.append(jnp.where(from_flat, pick(flat, source_at), pick(tall, source_at)))
        partner = []
        for b in range(4):
            w = found[3 - b]
            w = jnp.where(ec0, up(w, 2, 0), down(w, 2, 0))
            partner.append(jnp.where(flipped, w, found[b]))
        return partner

    def glue(v, partner):
        v = [list(row) for row in v]
        sides = []
        for j in range(4):
            a, b, p = v[0][j], v[3][j], partner[j]
            s = down(p, 4, 0)
            v[0][j] = a + jnp.where(edge_at[0], p, prev_row(b))
            v[3][j] = b + jnp.where(er1 & y_hi, s, next_row(a))
            q = jnp.where(er1, p, s)
            q = jnp.where(er == ec, q, jnp.where(er0, down(q, 2, 0), up(q, 2, 0)))
            sides.append(q)
        q0, q3 = sides[0], sides[3]
        sides[0], sides[3] = q0 + prev_row(q3), q3 + next_row(q0)
        for i in range(4):
            a, b, q = v[i][0], v[i][3], sides[i]
            v[i][0] = a + jnp.where(ec0 & x_lo, q, prev_col(b))
            v[i][3] = b + jnp.where(ec1 & x_hi, q, next_col(a))
        return v

    def assemble_one(v):
        return glue(v, rims(v))

    def assemble_pair(u, v):
        pu, pv = rims(u), rims(v)
        tu = [cosine * a - sine * b for a, b in zip(pu, pv)]
        tv = [sine * a + cosine * b for a, b in zip(pu, pv)]
        return glue(u, tu), glue(v, tv)

    def grid(flat):
        return [[flat[8 * (4 * i + j) : 8 * (4 * i + j) + 8] for j in range(4)] for i in range(4)]

    def receive(ref, planes):
        blocks_in = [ref[p] for p in planes]
        blocks_in += [blocks_in[0]] * (LANES // count - len(blocks_in))
        return grid(jnp.concatenate(blocks_in, axis=0).T)

    def put(ref, k, v):
        for i in range(4):
            for j in range(4):
                ref[k, i, j] = v[i][j]

    def take(ref, k):
        return [[ref[k, i, j] for j in range(4)] for i in range(4)]

    def each(fn, *vs):
        return [[fn(*(v[i][j] for v in vs)) for j in range(4)] for i in range(4)]

    def copy_to(at, src, dst, sem_s, sem_r):
        pltpu.make_async_remote_copy(
            src_ref=src,
            dst_ref=dst,
            send_sem=sem_s,
            recv_sem=sem_r,
            device_id=at,
            device_id_type=MESH,
        ).start()

    def all_of(ref, sem_s, sem_r, first=0, planes=None, rows=None):
        planes = ref.shape[0] if planes is None else planes
        part = ref.at[pl.ds(first, planes), pl.ds(0, rows or count - 1)]
        return pltpu.make_async_remote_copy(
            src_ref=part,
            dst_ref=part,
            send_sem=sem_s,
            recv_sem=sem_r,
            device_id=(g, y, lax.rem(x + 1, blocks)),
            device_id_type=MESH,
        )

    pairs = 2 * faces
    half = count // 2
    parts = ((2 * faces, faces), (0, 2 * faces))
    pl.semaphore_wait(barrier, count - 1)
    odd = lax.rem(y, 2) == 1
    even = jnp.logical_not(odd)

    def send_shapes(c):
        for d, at in towards([c]):
            if at[1] % 2 == 1:
                src, dst = send_geo.at[pl.ds(0, pairs)], got_geo.at[:, me]
                pl.when(d != me)(functools.partial(copy_to, at, src, dst, sem_s_geo.at[0], sem_r_geo.at[0]))

    def send_part(n, c):
        part = pl.ds(*parts[n])
        for d, at in towards([c]):
            src, dst = send.at[part, d], got.at[part, me]
            pl.when(d != me)(functools.partial(copy_to, at, src, dst, sem_s_in.at[n], sem_r_in.at[n]))

    def send_from(column):
        for kind, c in zip(IN_KINDS, map(int, IN_COLUMNS[column])):
            if kind == "g":
                send_shapes(c)
            else:
                send_part("tw".index(kind), c)

    for column in range(blocks):
        pl.when(x == column)(functools.partial(send_from, column))

    for q in range(3 * faces):
        got[q, pl.ds(me, 1), :] = send[q, pl.ds(me, 1), :]

    @pl.when(odd)
    def _():
        for q in range(pairs):
            got_geo[q, pl.ds(me, 1), :] = send_geo[pl.ds(q, 1), :]


    relay = pltpu.make_async_remote_copy(
        src_ref=got_geo,
        dst_ref=got_geo,
        send_sem=sem_s_geo.at[1],
        recv_sem=sem_r_geo.at[1],
        device_id=(g, y + 1 - 2 * lax.rem(y, 2), x),
        device_id_type=MESH,
    )

    def shapes(rows):
        return all_of(got_geo, sem_s_geo.at[0], sem_r_geo.at[0], rows=rows)

    @pl.when(odd)
    def _():
        shapes(count - 1).wait_recv()
        relay.start()

    pl.when(even)(relay.wait_recv)
    for p in range(2):
        both = receive(got_geo, range(p, pairs, 2))
        put(coef, 2 * p, each(lambda v: jnp.where(lev == 0, v, down(v, 1, 0)), both))
        put(coef, 2 * p + 1, each(lambda v: jnp.where(lev == 1, v, up(v, 1, 0)), both))
    put(coef, 3, each(lambda v: 1.0 / v, assemble_one(take(coef, 3))))

    def fields_in(k):
        return receive(got, range(k * faces, (k + 1) * faces))

    def scaled(v):
        return each(lambda a, b: a * b, v, take(coef, 3))

    def laplace_of(v):
        a, b, c = take(coef, 0), take(coef, 1), take(coef, 2)
        gx, gy = slope_x(v), slope_y(v)
        fx = each(lambda p, q, m, n: m * p + n * q, gx, gy, a, b)
        fy = each(lambda p, q, m, n: m * p + n * q, gx, gy, b, c)
        total = each(lambda p, q: p + q, slope_x(fx), slope_y(fy))
        return [[jnp.float32(weights[i] * weights[j]) * total[i][j] for j in range(4)] for i in range(4)]

    def finish(k, v):
        done = each(lambda s, a: s - hyper_coeff * a, take(section, k), v)
        turned = jnp.concatenate([done[i][j] for i in range(4) for j in range(4)], axis=0).T
        for f in range(faces):
            back[k * faces + f] = turned[f * count : (f + 1) * count]

    def send_back(n):
        part = pl.ds(*parts[n])
        for d, at in towards(range(blocks)):
            pl.when(d != me)(
                functools.partial(copy_to, at, back.at[part, d], out.at[part, me], sem_s_out, sem_r_out)
            )

    def kept(n):
        part = pl.ds(*parts[n])
        return pltpu.make_async_copy(back.at[part, me], out.at[part, me], sem_own.at[n])

    def arrived(n):
        first, planes = parts[n]
        return all_of(got, sem_s_in.at[n], sem_r_in.at[n], first, planes)

    arrived(0).wait_recv()
    heat = scaled(assemble_one(fields_in(2)))
    put(section, 2, heat)
    heat = scaled(assemble_one(laplace_of(heat)))
    heat = scaled(assemble_one(laplace_of(heat)))
    finish(2, heat)
    send_back(0)
    kept(0).start()
    arrived(1).wait_recv()
    wind_u, wind_v = assemble_pair(fields_in(0), fields_in(1))
    put(section, 0, scaled(wind_u))
    put(section, 1, scaled(wind_v))
    wind_u, wind_v = assemble_pair(laplace_of(take(section, 0)), laplace_of(take(section, 1)))
    wind_u, wind_v = assemble_pair(laplace_of(scaled(wind_u)), laplace_of(scaled(wind_v)))
    finish(0, scaled(wind_u))
    finish(1, scaled(wind_v))
    send_back(1)
    kept(1).start()

    @pl.when(odd)
    def _():
        shapes(half - 1).wait_send()
        relay.wait_send()

    pl.when(even)(shapes(half).wait_send)
    arrived(0).wait_send()
    arrived(1).wait_send()
    kept(0).wait()
    kept(1).wait()
    all_of(out, sem_s_out, sem_r_out).wait_send()
    all_of(out, sem_s_out, sem_r_out).wait_recv()


def last_kernel(got, out, mix, full, sem):
    faces = full.shape[0]
    lane = lax.broadcasted_iota(jnp.int32, (SIDE, LANES), 1)
    first = (lane // 32) % 2 == 0

    def half_rows(n, f, r, h):
        start = (r % 4) * 32 + (r // 4) * 4 + h
        return jnp.concatenate([mix[n, f, pl.ds(start + ec * 2, 4, stride=8), :] for ec in range(2)], axis=0)

    def copy_of(f):
        return pltpu.make_async_copy(full.at[f], out.at[f], sem.at[f])

    for f in range(faces):
        u, v, t = (got[k * faces + f] for k in range(3))
        for m, parts in enumerate(((u, u, v, v), (t, t, t, t))):
            mix[m, f] = jnp.concatenate(parts, axis=0).T
    for f in range(faces):
        for r in range(SIDE):
            wind, temp = (jnp.where(first, half_rows(m, f, r, 0), half_rows(m, f, r, 1)) for m in range(2))
            full[f, r, :, 0 : 2 * HALF] = wind
            full[f, r, :, 2 * HALF : 3 * HALF] = temp[:, 0:HALF]
        copy_of(f).start()
    for f in range(faces):
        copy_of(f).wait()


def by_level(groups, blocks, state, jacobian, metric_diag, metric_cross, coriolis, nbr_face, nbr_edge):
    faces = state.shape[0]
    count = groups * blocks * blocks
    vmem, anywhere = pl.BlockSpec(memory_space=pltpu.VMEM), pl.BlockSpec(memory_space=pl.ANY)
    inputs = (nbr_face.T, nbr_edge.T, state, jacobian, metric_diag, metric_cross, coriolis)
    inputs = [pltpu.with_memory_space_constraint(a, pltpu.HBM) for a in inputs]
    piece = (3 * faces, count, LANES)
    cells = (4, 4, SIDE, LANES)
    dma = pltpu.SemaphoreType.DMA
    got = pl.pallas_call(
        functools.partial(main_kernel, groups, blocks),
        out_shape=jax.ShapeDtypeStruct(piece, jnp.float32),
        in_specs=[pl.BlockSpec(memory_space=pltpu.HBM)] * 7,
        out_specs=anywhere,
        scratch_shapes=[pltpu.SMEM(a.shape, a.dtype) for a in inputs[:2]]
        + [pltpu.VMEM(a.shape, a.dtype) for a in inputs[2:]]
        + [
            pltpu.VMEM((faces + 1, LANES, LANES), jnp.float32),
            pltpu.VMEM(piece, jnp.float32),
            pltpu.VMEM((SIDE, LANES), jnp.float32),
            pltpu.VMEM(piece, jnp.float32),
            pltpu.VMEM((2 * faces, count, LANES), jnp.float32),
            pltpu.VMEM((4,) + cells, jnp.float32),
            pltpu.VMEM((3,) + cells, jnp.float32),
            pltpu.VMEM(piece, jnp.float32),
        ]
        + [dma((7,)), dma((2,)), dma((2,)), dma((2,)), dma((2,)), dma, dma, dma((3,))],
        compiler_params=pltpu.CompilerParams(collective_id=0, has_side_effects=True, vmem_limit_bytes=16 << 20),
    )(*inputs)
    return pl.pallas_call(
        last_kernel,
        out_shape=jax.ShapeDtypeStruct(state.shape, jnp.float32),
        in_specs=[vmem],
        out_specs=anywhere,
        scratch_shapes=[
            pltpu.VMEM((2, faces, LANES, LANES), jnp.float32),
            pltpu.VMEM(state.shape, jnp.float32),
            dma((faces,)),
        ],
        compiler_params=pltpu.CompilerParams(vmem_limit_bytes=16 << 20),
    )(got)


def solution(mesh):
    groups, rows, columns = (mesh.shape[axis] for axis in ("face", "fy", "fx"))
    count = groups * rows * columns

    def body(*args):
        state = args[0]
        faces = state.shape[0]
        fits = rows == columns == 4 and 2 * count == HALF and faces * count <= LANES
        if fits and state.shape[1:] == (SIDE, SIDE, 3 * HALF) and 2 * faces <= SIDE:
            return by_level(groups, rows, *args)
        return per_device(*args)

    return jax.shard_map(
        body,
        mesh=mesh,
        in_specs=(
            P("face", "fy", "fx", None),
            P("face", "fy", "fx"),
            P(None, "face", "fy", "fx"),
            P("face", "fy", "fx"),
            P("face", "fy", "fx"),
            P(),
            P(),
        ),
        out_specs=P("face", "fy", "fx", None),
        check_vma=False,
    )
```

```python
import functools

import jax
import jax.numpy as jnp
import numpy as np
from jax import lax
from jax.experimental import pallas as pl
from jax.experimental.pallas import tpu as pltpu
from jax.sharding import PartitionSpec as P

time_step = 0.05
hyper_coeff = 0.0005
MESH = pl.DeviceIdType.MESH


def padded(cells, sides, width):
    for axis, dim in sides:
        count = lax.axis_size(axis)
        ends = count - 1
        head = lax.slice_in_dim(cells, 0, width, axis=dim)
        tail = lax.slice_in_dim(cells, cells.shape[dim] - width, cells.shape[dim], axis=dim)
        cells = jnp.concatenate(
            [
                lax.ppermute(tail, axis, [(i, (i + 1) % count) for i in range(ends)]),
                cells,
                lax.ppermute(head, axis, [((i + 1) % count, i) for i in range(ends)]),
            ],
            axis=dim,
        )
    return cells


def deriv_table():
    gll_nodes = np.array([-1.0, -1.0 / np.sqrt(5.0), 1.0 / np.sqrt(5.0), 1.0])
    bary_weights = np.ones(4)
    for j in range(4):
        for m in range(4):
            if m != j:
                bary_weights[j] = bary_weights[j] / (gll_nodes[j] - gll_nodes[m])
    matrix = np.zeros((4, 4))
    for i in range(4):
        for j in range(4):
            if i != j:
                matrix[i, j] = bary_weights[j] / bary_weights[i] / (gll_nodes[i] - gll_nodes[j])
        matrix[i, i] = -np.sum(matrix[i])
    return matrix


def along_x(values):
    face_count, row_count, col_count, chan_count = values.shape
    blocks = values.reshape(face_count, row_count, col_count // 4, 4, chan_count)
    result = jnp.einsum(
        "jk,abekc->abejc",
        jnp.asarray(deriv_table(), jnp.float32),
        blocks,
        precision=lax.Precision.HIGHEST,
    )
    return result.reshape(values.shape)


def along_y(values):
    face_count, row_count, col_count, chan_count = values.shape
    blocks = values.reshape(face_count, row_count // 4, 4, col_count, chan_count)
    result = jnp.einsum(
        "ik,aekxc->aeixc",
        jnp.asarray(deriv_table(), jnp.float32),
        blocks,
        precision=lax.Precision.HIGHEST,
    )
    return result.reshape(values.shape)


def mass_of(jacobian):
    weights = jnp.asarray([1.0 / 6.0, 5.0 / 6.0, 5.0 / 6.0, 1.0 / 6.0], jnp.float32)
    row_weight = jnp.tile(weights, jacobian.shape[1] // 4)
    col_weight = jnp.tile(weights, jacobian.shape[2] // 4)
    return jacobian * row_weight[None, :, None] * col_weight[None, None, :]


def tendency(state, geometry, planet):
    volume, metric_xx, metric_yy, metric_xy = geometry
    levels = state.shape[-1] // 3
    wind_u = state[..., :levels]
    wind_v = state[..., levels : 2 * levels]
    temper = state[..., 2 * levels :]
    contra_u = metric_xx * wind_u + metric_xy * wind_v
    contra_v = metric_xy * wind_u + metric_yy * wind_v
    energy = 0.5 * (wind_u * contra_u + wind_v * contra_v) + temper
    xderivs = along_x(jnp.concatenate([wind_v, temper, energy], -1))
    yderivs = along_y(jnp.concatenate([wind_u, temper, energy], -1))
    absolute = (xderivs[..., :levels] - yderivs[..., :levels]) / volume + planet
    tend_u = absolute * volume * contra_v - xderivs[..., 2 * levels :]
    tend_v = -absolute * volume * contra_u - yderivs[..., 2 * levels :]
    tend_t = -(
        contra_u * xderivs[..., levels : 2 * levels] + contra_v * yderivs[..., levels : 2 * levels]
    )
    return state + time_step * jnp.concatenate([tend_u, tend_v, tend_t], -1)


def laplace(values, geometry):
    volume, metric_xx, metric_yy, metric_xy = geometry
    grad_x = along_x(values)
    grad_y = along_y(values)
    flux_x = volume * (metric_xx * grad_x + metric_xy * grad_y)
    flux_y = volume * (metric_xy * grad_x + metric_yy * grad_y)
    return (along_x(flux_x) + along_y(flux_y)) / volume


def combine(values, axis):
    length = values.shape[axis] - 2
    positions = jnp.arange(length)
    leading = (positions % 4 == 0).astype(jnp.float32)
    trailing = (positions % 4 == 3).astype(jnp.float32)
    broad_shape = [1, 1, 1, 1]
    broad_shape[axis] = length
    leading = leading.reshape(broad_shape)
    trailing = trailing.reshape(broad_shape)
    middle = lax.slice_in_dim(values, 1, length + 1, axis=axis)
    previous = lax.slice_in_dim(values, 0, length, axis=axis)
    following = lax.slice_in_dim(values, 2, length + 2, axis=axis)
    return middle + leading * previous + trailing * following


def rotate(segment, quarter, levels):
    cosine = ((quarter == 0).astype(jnp.float32) - (quarter == 2).astype(jnp.float32))[..., None]
    sine_part = ((quarter == 1).astype(jnp.float32) - (quarter == 3).astype(jnp.float32))[..., None]
    wind_u = segment[..., :levels]
    wind_v = segment[..., levels : 2 * levels]
    return jnp.concatenate(
        [
            cosine * wind_u - sine_part * wind_v,
            sine_part * wind_u + cosine * wind_v,
            segment[..., 2 * levels :],
        ],
        -1,
    )


def in_face(values):
    across = combine(padded(values, (("fx", 2),), 1), 2)
    return combine(padded(across, (("fy", 1),), 1), 1)


def place_pieces(
    got_flat,
    got_tall,
    vector,
    nbr_edge,
    flat_edge,
    tall_edge,
    on_south,
    on_west,
    flat_start,
    tall_start,
    face_local,
    side_nodes,
    chan_count,
    levels,
):
    edge_ids = jnp.arange(4, dtype=jnp.int32)
    flat_target = nbr_edge[:, flat_edge]
    tall_target = nbr_edge[:, tall_edge]
    if vector:
        got_flat = rotate(got_flat, ((flat_target - flat_edge + 2) % 4)[None, :, None], levels)
        got_tall = rotate(got_tall, ((tall_target - tall_edge + 2) % 4)[None, :, None], levels)
    got_flat = jnp.where(on_south, got_flat[:, :, ::-1], got_flat)
    got_tall = jnp.where(on_west, got_tall, got_tall[:, :, ::-1])
    flat_pick = (flat_target[:, None] == edge_ids[None, :]).astype(jnp.float32)
    tall_pick = (tall_target[:, None] == edge_ids[None, :]).astype(jnp.float32)
    flat_rims = jnp.einsum("se,gsjc->gejc", flat_pick, got_flat, precision=lax.Precision.HIGHEST)
    tall_rims = jnp.einsum("se,gsjc->gejc", tall_pick, got_tall, precision=lax.Precision.HIGHEST)
    empty_rims = jnp.zeros((face_local, 4, side_nodes, chan_count), jnp.float32)
    rim_strips = lax.dynamic_update_slice(empty_rims, flat_rims, (0, 0, flat_start, 0))
    return rim_strips + lax.dynamic_update_slice(empty_rims, tall_rims, (0, 0, tall_start, 0))


def outgoing(
    summed, nbr_face, face_ids, flat_edge, tall_edge, on_south, on_west, flat_live, tall_live
):
    row_count = summed.shape[1]
    col_count = summed.shape[2]
    all_faces = jnp.arange(nbr_face.shape[0], dtype=jnp.int32)
    flat_piece = jnp.where(on_south, summed[:, 0], summed[:, row_count - 1])
    tall_piece = jnp.where(on_west, summed[:, :, 0], summed[:, :, col_count - 1])
    flat_dest = nbr_face[face_ids, flat_edge]
    tall_dest = nbr_face[face_ids, tall_edge]
    flat_send = ((all_faces[:, None] == flat_dest[None, :]) & flat_live).astype(jnp.float32)
    tall_send = ((all_faces[:, None] == tall_dest[None, :]) & tall_live).astype(jnp.float32)
    return (
        flat_send[:, :, None, None] * flat_piece[None],
        tall_send[:, :, None, None] * tall_piece[None],
    )


def assemble(values, vector, nbr_face, nbr_edge):
    summed = in_face(values)
    face_local, row_count, col_count, chan_count = summed.shape
    levels = chan_count // 3
    row_index = lax.axis_index("fy")
    col_index = lax.axis_index("fx")
    side_nodes = row_count * lax.axis_size("fy")
    face_ids = lax.axis_index("face") * face_local + jnp.arange(face_local, dtype=jnp.int32)
    on_south = row_index == 0
    on_north = row_index == lax.axis_size("fy") - 1
    on_west = col_index == 0
    on_east = col_index == lax.axis_size("fx") - 1
    flat_live = on_south | on_north
    tall_live = on_west | on_east
    flat_edge = jnp.where(on_south, 0, 2).astype(jnp.int32)
    tall_edge = jnp.where(on_west, 3, 1).astype(jnp.int32)
    flat_start = jnp.where(
        on_south, side_nodes - (col_index + 1) * col_count, col_index * col_count
    )
    tall_start = jnp.where(on_west, row_index * row_count, side_nodes - (row_index + 1) * row_count)
    send_flat, send_tall = outgoing(
        summed, nbr_face, face_ids, flat_edge, tall_edge, on_south, on_west, flat_live, tall_live
    )
    got_flat, got_tall = (
        lax.all_to_all(send_flat, "face", split_axis=0, concat_axis=1, tiled=True),
        lax.all_to_all(send_tall, "face", split_axis=0, concat_axis=1, tiled=True),
    )
    rim_strips = place_pieces(
        got_flat,
        got_tall,
        vector,
        nbr_edge,
        flat_edge,
        tall_edge,
        on_south,
        on_west,
        flat_start,
        tall_start,
        face_local,
        side_nodes,
        chan_count,
        levels,
    )
    flat_lines = jnp.stack([rim_strips[:, 0], rim_strips[:, 2, ::-1]], axis=1)
    flat_lines = flat_lines.reshape(face_local, 2, lax.axis_size("fx"), col_count, chan_count)
    tall_lines = jnp.stack([rim_strips[:, 1], rim_strips[:, 3, ::-1]], axis=1)
    tall_lines = tall_lines.reshape(face_local, 2, lax.axis_size("fy"), row_count, chan_count)
    flat_whole = lax.psum(flat_lines, "fy")
    tall_whole = lax.psum(tall_lines, "fx")
    flat_block = lax.psum_scatter(flat_whole, "fx", scatter_dimension=2, tiled=True)
    tall_block = lax.psum_scatter(tall_whole, "fy", scatter_dimension=2, tiled=True)
    flat_add = jnp.where(on_south, flat_block[:, 0, 0], flat_block[:, 1, 0])
    tall_add = jnp.where(on_west, tall_block[:, 1, 0], tall_block[:, 0, 0])
    result = summed.at[:, 0].add(jnp.where(on_south, flat_add, 0.0))
    result = result.at[:, row_count - 1].add(jnp.where(on_north, flat_add, 0.0))
    result = result.at[:, :, 0].add(jnp.where(on_west, tall_add, 0.0))
    result = result.at[:, :, col_count - 1].add(jnp.where(on_east, tall_add, 0.0))
    return result


def per_device(state, jacobian, metric_diag, metric_cross, coriolis, nbr_face, nbr_edge):
    node_mass = mass_of(jacobian)[..., None]
    total_mass = assemble(node_mass, False, nbr_face, nbr_edge)
    geometry = (
        jacobian[..., None],
        metric_diag[0][..., None],
        metric_diag[1][..., None],
        metric_cross[..., None],
    )
    raw = tendency(state, geometry, coriolis[..., None])
    sectioned = assemble(node_mass * raw, True, nbr_face, nbr_edge) / total_mass
    first_lap = (
        assemble(node_mass * laplace(sectioned, geometry), True, nbr_face, nbr_edge) / total_mass
    )
    second_lap = (
        assemble(node_mass * laplace(first_lap, geometry), True, nbr_face, nbr_edge) / total_mass
    )
    return sectioned - hyper_coeff * second_lap


SIDE = 8
HALF = 64
LANES = 128


IN_KINDS = "gggtttwwwgtw"
IN_COLUMNS = ("321321321000", "320320320111", "301301301222", "012012012333")


def up(v, count, axis):
    return pltpu.roll(v, v.shape[axis] - count, axis)


def down(v, count, axis):
    return pltpu.roll(v, count, axis)


def slope_size():
    d = deriv_table()
    return (d[0, 0] + d[0, 3]) / 2


def slope(a, size=1.0):
    d = deriv_table() / (2 * size)
    p0, p1, m0, m1 = a[0] + a[3], a[1] + a[2], a[0] - a[3], a[1] - a[2]
    bend = p0 - p1
    o0 = bend if size != 1.0 else jnp.float32(d[0, 0] + d[0, 3]) * bend
    o1 = jnp.float32(d[1, 0] + d[1, 3]) * bend
    q0 = jnp.float32(d[0, 0] - d[0, 3]) * m0 + jnp.float32(d[0, 1] - d[0, 2]) * m1
    q1 = jnp.float32(d[1, 0] - d[1, 3]) * m0 + jnp.float32(d[1, 1] - d[1, 2]) * m1
    return [q0 + o0, q1 + o1, q1 - o1, q0 - o0]


def slope_x(v):
    return [slope(v[i], slope_size()) for i in range(4)]


def slope_y(v):
    cols = [slope([v[i][j] for i in range(4)], slope_size()) for j in range(4)]
    return [[cols[j][i] for j in range(4)] for i in range(4)]


def spread(mix, plane, er, i, which, v):
    for ec in range(2):
        mix[plane, pl.ds(er * 64 + ec * 32 + which * 16 + i * 4, 4), :] = v[4 * ec : 4 * ec + 4]


def by_node(mix, plane):
    return jnp.concatenate([mix[plane, pl.ds(n, 8, stride=16), :] for n in range(16)], axis=0)


def main_kernel(
    groups,
    blocks,
    nbr_face_in,
    nbr_edge_in,
    state_in,
    jac_in,
    diag_in,
    cross_in,
    coriolis_in,
    out,
    nbr_face,
    nbr_edge,
    state,
    jac,
    diag,
    cross,
    coriolis,
    mix,
    send,
    send_geo,
    got,
    got_geo,
    coef,
    section,
    back,
    sem_load,
    sem_s_geo,
    sem_r_geo,
    sem_s_in,
    sem_r_in,
    sem_s_out,
    sem_r_out,
    sem_own,
):
    faces = state.shape[0]
    count = groups * blocks * blocks
    last = blocks - 1
    g = lax.axis_index("face")
    y = lax.axis_index("fy")
    x = lax.axis_index("fx")
    me = (g * blocks + y) * blocks + x

    def by_distance(at):
        return [last - at, lax.rem(at + 2, 4), at + 1 - 2 * lax.rem(at, 2), at]

    def others(columns):
        for n, tx in enumerate(columns):
            for ty in by_distance(y)[: blocks - 1] + [y]:
                for tg in (lax.rem(g + 1, groups), g):
                    if tx is not x or ty is not y or tg is not g:
                        yield (tg * blocks + ty) * blocks + tx, (tg, ty, tx)

    def towards(columns):
        for tx in columns:
            for ty in range(blocks):
                for tg in range(groups):
                    yield (tg * blocks + ty) * blocks + tx, (tg, ty, tx)

    loads = [
        pltpu.make_async_copy(src, dst, sem_load.at[n])
        for n, (src, dst) in enumerate(
            (
                (state_in, state),
                (jac_in, jac),
                (diag_in, diag),
                (cross_in, cross),
                (coriolis_in, coriolis),
                (nbr_face_in, nbr_face),
                (nbr_edge_in, nbr_edge),
            )
        )
    ]
    barrier = pltpu.get_barrier_semaphore()
    for _, at in others(by_distance(x)):
        pl.semaphore_signal(barrier, inc=1, device_id=at, device_id_type=MESH)
    for load in loads:
        load.start()
    for load in loads[1:]:
        load.wait()

    sub = lax.broadcasted_iota(jnp.int32, (SIDE, LANES), 0)
    lane = lax.broadcasted_iota(jnp.int32, (SIDE, LANES), 1)
    low = lane < HALF
    node = sub % 4
    table = deriv_table()
    weights = (1.0 / 6.0, 5.0 / 6.0, 5.0 / 6.0, 1.0 / 6.0)
    zero = jnp.zeros((SIDE, LANES), jnp.float32)

    def per_node(entries, at):
        total = jnp.full(at.shape, entries[0], jnp.float32)
        for n in range(1, 4):
            total = jnp.where(at == n, jnp.float32(entries[n]), total)
        return total

    taps = {
        s: per_node([float(table[n, n + s]) if 0 <= n + s < 4 else 0.0 for n in range(4)], node)
        for s in range(-3, 4)
    }

    def swap(v):
        return pltpu.roll(v, HALF, 1)

    def along_sub(v):
        total = taps[0] * v
        for s in (-3, -2, -1, 1, 2, 3):
            total = total + taps[s] * pltpu.roll(v, (-s) % SIDE, 0)
        return total

    def pick(v, at):
        return jnp.take_along_axis(v, at, axis=1, mode="promise_in_bounds")

    def spread_lanes(tiles):
        tiles = tiles + [tiles[0]] * (LANES // SIDE - len(tiles))
        return jnp.concatenate(tiles, axis=0).T

    tile_sub = lax.broadcasted_iota(jnp.int32, (SIDE, SIDE), 0) % 4
    tile_lane = lax.broadcasted_iota(jnp.int32, (SIDE, SIDE), 1) % 4
    tile_weight = per_node(weights, tile_sub) * per_node(weights, tile_lane)
    near_tiles, far_tiles = [], []
    for f in range(faces):
        vol, m_xx, m_yy, m_xy = jac[f], diag[0, f], diag[1, f], cross[f]
        mass = vol * tile_weight
        near_tiles += [m_xx, m_yy, m_xy, vol * coriolis[f], mass]
        far_tiles += [vol * m_xx, vol * m_yy, vol * m_xy, mass]
    local, shared = spread_lanes(near_tiles), spread_lanes(far_tiles)

    def spot(f, k, r):
        return (f * 5 + k) * SIDE + r

    cells = [(f, r) for f in range(faces) for r in range(SIDE)]
    lines = [[n + i for i in range(4)] for n in range(0, len(cells), 4)]
    for r in range(SIDE):
        for h in range(2):
            at = (lane // 2 % faces) * (4 * SIDE) + (2 * h + lane % 2) * SIDE + r
            spread(mix, faces, r // 4, r % 4, h, pick(shared, at))
    own = [pick(local, jnp.where(low, spot(f, 0, r), spot(f, 1, r))) for f, r in cells]
    skew = [pick(local, lane * 0 + spot(f, 2, r)) for f, r in cells]
    turn = [pick(local, lane * 0 + spot(f, 3, r)) for f, r in cells]
    mass = [pick(local, lane * 0 + spot(f, 4, r)) for f, r in cells]
    send_geo[...] = by_node(mix, faces).T[0:SIDE]
    loads[0].wait()
    wind = [state[f, r, :, 0 : 2 * HALF] for f, r in cells]
    temp = [state[f, r, :, 2 * HALF : 3 * HALF] for f, r in cells]
    temp = [jnp.concatenate([t, t], axis=1) for t in temp]
    other = [swap(w) for w in wind]
    contra = [m * w + n * o for m, n, w, o in zip(own, skew, wind, other)]
    power = [w * c for w, c in zip(wind, contra)]
    crossed = [swap(c) for c in contra]
    turned = [swap(p) for p in power]
    energy = [0.5 * (p + q) + t for p, q, t in zip(power, turned, temp)]

    def down_lines(v):
        out = [None] * len(cells)
        for line in lines:
            for n, d in zip(line, slope([v[n] for n in line])):
                out[n] = d
        return out

    dxs = [along_sub(jnp.where(low, e, w)) for e, w in zip(energy, wind)]
    dys = down_lines([jnp.where(low, w, e) for e, w in zip(energy, wind)])
    flow = [c * jnp.where(low, a, b) for c, a, b in zip(contra, [along_sub(t) for t in temp], down_lines(temp))]
    dxv = [swap(a) for a in dxs]
    dyu = [swap(a) for a in dys]
    flow = [q + swap(q) for q in flow]
    heat = [m * (t - time_step * q) for m, t, q in zip(mass, temp, flow)]
    fresh = []
    for n in range(len(cells)):
        spin = jnp.where(low, dxv[n] - dys[n], dyu[n] - dxs[n]) + jnp.where(low, turn[n], -turn[n])
        tend = spin * crossed[n] - jnp.where(low, dxs[n], dys[n])
        fresh.append(mass[n] * (wind[n] + time_step * tend))
    second = (lane >= 32) & (lane < 64)
    shifted = [(down(t, 32, 1), up(w, 32, 1)) for t, w in zip(heat, fresh)]
    for n, (f, r) in enumerate(cells):
        spread(mix, f, r // 4, r % 4, 0, jnp.where(second, shifted[n][0], fresh[n]))
        spread(mix, f, r // 4, r % 4, 1, jnp.where(second, heat[n], shifted[n][1]))
    for f in range(faces):
        turned = by_node(mix, f).T
        for k, part in enumerate((0, 2, 1)):
            send[k * faces + f] = turned[part * count : (part + 1) * count]

    er, ec, lev = sub // 4, (sub // 2) % 2, sub % 2
    lx, ly = lane % blocks, (lane // blocks) % blocks
    panel = lane // (blocks * blocks)
    er0, er1, ec0, ec1 = er == 0, er == 1, ec == 0, ec == 1
    x_lo, x_hi, y_lo, y_hi = lx == 0, lx == last, ly == 0, ly == last
    edge_at = (er0 & y_lo, er1 & x_hi, er0 & y_hi, er1 & x_lo)

    first_at = jnp.zeros((SIDE, LANES), jnp.int32)
    step_at, quarter_at = first_at, first_at
    for e in range(4):
        firsts, steps, quarters = first_at * 0, first_at * 0, first_at * 0
        for f in range(faces):
            for k in range(groups):
                nf = nbr_face[e, k * faces + f]
                ne = nbr_edge[e, k * faces + f]
                nl, ng = nf % faces, nf // faces
                tall = ne % 2
                step = 1 + tall * (blocks - 1)
                flips = jnp.where(ne >= 2, 0 if e < 2 else 1, 1 if e < 2 else 0)
                offset = jnp.where(ne == 2, last * blocks, jnp.where(ne == 1, last, 0))
                first = (nl * groups + ng) * (blocks * blocks) + offset + flips * (last * step)
                here = panel == f * groups + k
                firsts = jnp.where(here, first, firsts)
                steps = jnp.where(here, step * (1 - 2 * flips), steps)
                quarters = jnp.where(here, (e - ne + 2 + 4) % 4, quarters)
        first_at = jnp.where(edge_at[e], firsts, first_at)
        step_at = jnp.where(edge_at[e], steps, step_at)
        quarter_at = jnp.where(edge_at[e], quarters, quarter_at)
    source_at = first_at + step_at * jnp.where(er0, lx, ly)
    flipped = step_at < 0
    from_flat = (step_at == 1) | (step_at == -1)
    cosine = jnp.where(quarter_at == 0, 1.0, jnp.where(quarter_at == 2, -1.0, 0.0))
    sine = jnp.where(quarter_at == 1, 1.0, jnp.where(quarter_at == 3, -1.0, 0.0))

    def next_row(v):
        s = down(v, 4, 0)
        return jnp.where(er0, s, jnp.where(y_hi, zero, up(s, blocks, 1)))

    def prev_row(v):
        s = down(v, 4, 0)
        return jnp.where(er1, s, jnp.where(y_lo, zero, down(s, blocks, 1)))

    def next_col(v):
        return jnp.where(ec0, up(v, 2, 0), jnp.where(x_hi, zero, up(down(v, 2, 0), 1, 1)))

    def prev_col(v):
        return jnp.where(ec1, down(v, 2, 0), jnp.where(x_lo, zero, down(up(v, 2, 0), 1, 1)))

    def rims(v):
        found = []
        for b in range(4):
            flat = jnp.where(y_hi, v[3][b], v[0][b])
            flat = jnp.where(er0 == y_hi, down(flat, 4, 0), flat)
            tall = jnp.where(x_hi, v[b][3], v[b][0])
            tall = jnp.where(ec0 == x_hi, jnp.where(x_hi, up(tall, 2, 0), down(tall, 2, 0)), tall)
            tall = jnp.where(er == ec, tall, down(tall, 4, 0))
            found.append(jnp.where(from_flat, pick(flat, source_at), pick(tall, source_at)))
        partner = []
        for b in range(4):
            w = found[3 - b]
            w = jnp.where(ec0, up(w, 2, 0), down(w, 2, 0))
            partner.append(jnp.where(flipped, w, found[b]))
        return partner

    def glue(v, partner):
        v = [list(row) for row in v]
        sides = []
        for j in range(4):
            a, b, p = v[0][j], v[3][j], partner[j]
            s = down(p, 4, 0)
            v[0][j] = a + jnp.where(edge_at[0], p, prev_row(b))
            v[3][j] = b + jnp.where(er1 & y_hi, s, next_row(a))
            q = jnp.where(er1, p, s)
            q = jnp.where(er == ec, q, jnp.where(er0, down(q, 2, 0), up(q, 2, 0)))
            sides.append(q)
        q0, q3 = sides[0], sides[3]
        sides[0], sides[3] = q0 + prev_row(q3), q3 + next_row(q0)
        for i in range(4):
            a, b, q = v[i][0], v[i][3], sides[i]
            v[i][0] = a + jnp.where(ec0 & x_lo, q, prev_col(b))
            v[i][3] = b + jnp.where(ec1 & x_hi, q, next_col(a))
        return v

    ahead_of = jnp.where(er0, lx, ly)
    starts = ec0 & (ahead_of == 0)
    ends = ec1 & (ahead_of == last)
    before_at = jnp.where(starts, source_at, source_at - jnp.where(ec0, step_at, 0))
    after_at = jnp.where(ends, source_at, source_at + jnp.where(ec1, step_at, 0))
    up_lane, down_lane = jnp.where(er1, blocks, 0), jnp.where(er0, blocks, 0)
    right_lane, left_lane = jnp.where(ec1, 1, 0), jnp.where(ec0, 1, 0)

    def inside(at):
        return jnp.minimum(jnp.maximum(at, 0), LANES - 1)

    corner_at = (
        (inside(lane - down_lane - left_lane), inside(lane - down_lane + right_lane)),
        (inside(lane + up_lane - left_lane), inside(lane + up_lane + right_lane)),
    )

    def flip_col(v):
        return jnp.where(ec0, up(v, 2, 0), down(v, 2, 0))

    def rims_once(v):
        flats, talls = [], []
        for b in range(4):
            flat = jnp.where(y_hi, v[3][b], v[0][b])
            flats.append(jnp.where(er0 == y_hi, down(flat, 4, 0), flat))
            tall = jnp.where(x_hi, v[b][3], v[b][0])
            tall = jnp.where(ec0 == x_hi, jnp.where(x_hi, up(tall, 2, 0), down(tall, 2, 0)), tall)
            talls.append(jnp.where(er == ec, tall, down(tall, 4, 0)))

        def found(flat, tall, at):
            return jnp.where(from_flat, pick(flat, at), pick(tall, at))

        here = [found(flats[b], talls[b], source_at) for b in range(4)]
        partner = [jnp.where(flipped, flip_col(here[3 - b]), here[b]) for b in range(4)]
        turned = [(flip_col(flats[b]), flip_col(talls[b])) for b in range(4)]
        before = jnp.where(flipped, found(flats[0], talls[0], before_at), found(*turned[3], before_at))
        after = jnp.where(flipped, found(flats[3], talls[3], after_at), found(*turned[0], after_at))
        return partner + [jnp.where(starts, zero, before), jnp.where(ends, zero, after)]

    def glue_once(v, partner):
        x00, x03, x30, x33 = v[0][0], v[0][3], v[3][0], v[3][3]
        before, after = partner[4:]
        high = er1 & y_hi

        def diagonal(a, n, m):
            return pick(flip_col(down(a, 4, 0)), corner_at[n][m])

        corners = (
            (jnp.where(edge_at[0], before, diagonal(x33, 0, 0)), jnp.where(edge_at[0], after, diagonal(x30, 0, 1))),
            (
                jnp.where(high, down(before, 4, 0), diagonal(x03, 1, 0)),
                jnp.where(high, down(after, 4, 0), diagonal(x00, 1, 1)),
            ),
        )
        cols = [(prev_col(row[3]), next_col(row[0])) for row in v]
        rows = [(prev_row(v[3][j]), next_row(v[0][j])) for j in range(4)]
        v = [list(row) for row in v]
        sums = [partner[0] + before, partner[1], partner[2], partner[3] + after]
        for j in range(4):
            p = partner[j]
            v[0][j] = v[0][j] + jnp.where(edge_at[0], p, rows[j][0])
            v[3][j] = v[3][j] + jnp.where(high, down(p, 4, 0), rows[j][1])
        for i in range(4):
            p = sums[i]
            q = jnp.where(er1, p, down(p, 4, 0))
            q = jnp.where(er == ec, q, jnp.where(er0, down(q, 2, 0), up(q, 2, 0)))
            left, right = cols[i]
            if i in (0, 3):
                left, right = left + corners[i // 3][0], right + corners[i // 3][1]
            v[i][0] = v[i][0] + jnp.where(ec0 & x_lo, q, left)
            v[i][3] = v[i][3] + jnp.where(ec1 & x_hi, q, right)
        return v

    def assemble_one(v):
        return glue_once(v, rims_once(v))

    def assemble_pair(u, v):
        pu, pv = rims(u), rims(v)
        tu = [cosine * a - sine * b for a, b in zip(pu, pv)]
        tv = [sine * a + cosine * b for a, b in zip(pu, pv)]
        return glue(u, tu), glue(v, tv)

    def grid(flat):
        return [[flat[8 * (4 * i + j) : 8 * (4 * i + j) + 8] for j in range(4)] for i in range(4)]

    def receive(ref, planes):
        blocks_in = [ref[p] for p in planes]
        blocks_in += [blocks_in[0]] * (LANES // count - len(blocks_in))
        return grid(jnp.concatenate(blocks_in, axis=0).T)

    def put(ref, k, v):
        for i in range(4):
            for j in range(4):
                ref[k, i, j] = v[i][j]

    def take(ref, k):
        return [[ref[k, i, j] for j in range(4)] for i in range(4)]

    def each(fn, *vs):
        return [[fn(*(v[i][j] for v in vs)) for j in range(4)] for i in range(4)]

    def copy_to(at, src, dst, sem_s, sem_r):
        pltpu.make_async_remote_copy(
            src_ref=src,
            dst_ref=dst,
            send_sem=sem_s,
            recv_sem=sem_r,
            device_id=at,
            device_id_type=MESH,
        ).start()

    def all_of(ref, sem_s, sem_r, first=0, planes=None, rows=None):
        planes = ref.shape[0] if planes is None else planes
        part = ref.at[pl.ds(first, planes), pl.ds(0, rows or count - 1)]
        return pltpu.make_async_remote_copy(
            src_ref=part,
            dst_ref=part,
            send_sem=sem_s,
            recv_sem=sem_r,
            device_id=(g, y, lax.rem(x + 1, blocks)),
            device_id_type=MESH,
        )

    pairs = 2 * faces
    half = count // 2
    parts = ((2 * faces, faces), (0, 2 * faces))
    pl.semaphore_wait(barrier, count - 1)
    odd = lax.rem(y, 2) == 1
    even = jnp.logical_not(odd)

    def send_shapes(c):
        for d, at in towards([c]):
            if at[1] % 2 == 1:
                src, dst = send_geo.at[pl.ds(0, pairs)], got_geo.at[:, me]
                pl.when(d != me)(functools.partial(copy_to, at, src, dst, sem_s_geo.at[0], sem_r_geo.at[0]))

    def send_part(n, c):
        part = pl.ds(*parts[n])
        for d, at in towards([c]):
            src, dst = send.at[part, d], got.at[part, me]
            pl.when(d != me)(functools.partial(copy_to, at, src, dst, sem_s_in.at[n], sem_r_in.at[n]))

    def send_from(column):
        for kind, c in zip(IN_KINDS, map(int, IN_COLUMNS[column])):
            if kind == "g":
                send_shapes(c)
            else:
                send_part("tw".index(kind), c)

    for column in range(blocks):
        pl.when(x == column)(functools.partial(send_from, column))

    for q in range(3 * faces):
        got[q, pl.ds(me, 1), :] = send[q, pl.ds(me, 1), :]

    @pl.when(odd)
    def _():
        for q in range(pairs):
            got_geo[q, pl.ds(me, 1), :] = send_geo[pl.ds(q, 1), :]


    relay = pltpu.make_async_remote_copy(
        src_ref=got_geo,
        dst_ref=got_geo,
        send_sem=sem_s_geo.at[1],
        recv_sem=sem_r_geo.at[1],
        device_id=(g, y + 1 - 2 * lax.rem(y, 2), x),
        device_id_type=MESH,
    )

    def shapes(rows):
        return all_of(got_geo, sem_s_geo.at[0], sem_r_geo.at[0], rows=rows)

    @pl.when(odd)
    def _():
        shapes(count - 1).wait_recv()
        relay.start()

    pl.when(even)(relay.wait_recv)
    for p in range(2):
        both = receive(got_geo, range(p, pairs, 2))
        put(coef, 2 * p, each(lambda v: jnp.where(lev == 0, v, down(v, 1, 0)), both))
        put(coef, 2 * p + 1, each(lambda v: jnp.where(lev == 1, v, up(v, 1, 0)), both))
    inverse = each(lambda v: 1.0 / v, assemble_one(take(coef, 3)))
    put(coef, 3, inverse)
    unit = [[jnp.float32(slope_size() ** 2 * weights[i] * weights[j]) for j in range(4)] for i in range(4)]
    put(coef, 4, [[unit[i][j] * inverse[i][j] for j in range(4)] for i in range(4)])

    def fields_in(k):
        return receive(got, range(k * faces, (k + 1) * faces))

    def scaled(v, by=4):
        return each(lambda a, b: a * b, v, take(coef, by))

    def laplace_of(v):
        a, b, c = take(coef, 0), take(coef, 1), take(coef, 2)
        gx, gy = slope_x(v), slope_y(v)
        fx = each(lambda p, q, m, n: m * p + n * q, gx, gy, a, b)
        fy = each(lambda p, q, m, n: m * p + n * q, gx, gy, b, c)
        return each(lambda p, q: p + q, slope_x(fx), slope_y(fy))

    def finish(k, v):
        done = each(lambda s, a: s - hyper_coeff * a, take(section, k), v)
        turned = jnp.concatenate([done[i][j] for i in range(4) for j in range(4)], axis=0).T
        for f in range(faces):
            back[k * faces + f] = turned[f * count : (f + 1) * count]

    def send_back(n):
        part = pl.ds(*parts[n])
        for d, at in towards(range(blocks)):
            pl.when(d != me)(
                functools.partial(copy_to, at, back.at[part, d], out.at[part, me], sem_s_out, sem_r_out)
            )

    def kept(n):
        part = pl.ds(*parts[n])
        return pltpu.make_async_copy(back.at[part, me], out.at[part, me], sem_own.at[n])

    def arrived(n):
        first, planes = parts[n]
        return all_of(got, sem_s_in.at[n], sem_r_in.at[n], first, planes)

    arrived(0).wait_recv()
    heat = scaled(assemble_one(fields_in(2)), 3)
    put(section, 2, heat)
    heat = scaled(assemble_one(laplace_of(heat)))
    heat = scaled(assemble_one(laplace_of(heat)))
    finish(2, heat)
    send_back(0)
    kept(0).start()
    arrived(1).wait_recv()
    wind_u, wind_v = assemble_pair(fields_in(0), fields_in(1))
    put(section, 0, scaled(wind_u, 3))
    put(section, 1, scaled(wind_v, 3))
    wind_u, wind_v = assemble_pair(laplace_of(take(section, 0)), laplace_of(take(section, 1)))
    wind_u, wind_v = assemble_pair(laplace_of(scaled(wind_u)), laplace_of(scaled(wind_v)))
    finish(0, scaled(wind_u))
    finish(1, scaled(wind_v))
    send_back(1)
    kept(1).start()

    @pl.when(odd)
    def _():
        shapes(half - 1).wait_send()
        relay.wait_send()

    pl.when(even)(shapes(half).wait_send)
    arrived(0).wait_send()
    arrived(1).wait_send()
    kept(0).wait()
    kept(1).wait()
    all_of(out, sem_s_out, sem_r_out).wait_send()
    all_of(out, sem_s_out, sem_r_out).wait_recv()


def last_kernel(got, out, mix, full, sem):
    faces = full.shape[0]
    lane = lax.broadcasted_iota(jnp.int32, (SIDE, LANES), 1)
    first = (lane // 32) % 2 == 0

    def half_rows(n, f, r, h):
        start = (r % 4) * 32 + (r // 4) * 4 + h
        return jnp.concatenate([mix[n, f, pl.ds(start + ec * 2, 4, stride=8), :] for ec in range(2)], axis=0)

    def copy_of(f):
        return pltpu.make_async_copy(full.at[f], out.at[f], sem.at[f])

    for f in range(faces):
        u, v, t = (got[k * faces + f] for k in range(3))
        for m, parts in enumerate(((u, u, v, v), (t, t, t, t))):
            mix[m, f] = jnp.concatenate(parts, axis=0).T
    for f in range(faces):
        for r in range(SIDE):
            wind, temp = (jnp.where(first, half_rows(m, f, r, 0), half_rows(m, f, r, 1)) for m in range(2))
            full[f, r, :, 0 : 2 * HALF] = wind
            full[f, r, :, 2 * HALF : 3 * HALF] = temp[:, 0:HALF]
        copy_of(f).start()
    for f in range(faces):
        copy_of(f).wait()


def by_level(groups, blocks, state, jacobian, metric_diag, metric_cross, coriolis, nbr_face, nbr_edge):
    faces = state.shape[0]
    count = groups * blocks * blocks
    vmem, anywhere = pl.BlockSpec(memory_space=pltpu.VMEM), pl.BlockSpec(memory_space=pl.ANY)
    inputs = (nbr_face.T, nbr_edge.T, state, jacobian, metric_diag, metric_cross, coriolis)
    inputs = [pltpu.with_memory_space_constraint(a, pltpu.HBM) for a in inputs]
    piece = (3 * faces, count, LANES)
    cells = (4, 4, SIDE, LANES)
    dma = pltpu.SemaphoreType.DMA
    got = pl.pallas_call(
        functools.partial(main_kernel, groups, blocks),
        out_shape=jax.ShapeDtypeStruct(piece, jnp.float32),
        in_specs=[pl.BlockSpec(memory_space=pltpu.HBM)] * 7,
        out_specs=anywhere,
        scratch_shapes=[pltpu.SMEM(a.shape, a.dtype) for a in inputs[:2]]
        + [pltpu.VMEM(a.shape, a.dtype) for a in inputs[2:]]
        + [
            pltpu.VMEM((faces + 1, LANES, LANES), jnp.float32),
            pltpu.VMEM(piece, jnp.float32),
            pltpu.VMEM((SIDE, LANES), jnp.float32),
            pltpu.VMEM(piece, jnp.float32),
            pltpu.VMEM((2 * faces, count, LANES), jnp.float32),
            pltpu.VMEM((5,) + cells, jnp.float32),
            pltpu.VMEM((3,) + cells, jnp.float32),
            pltpu.VMEM(piece, jnp.float32),
        ]
        + [dma((7,)), dma((2,)), dma((2,)), dma((2,)), dma((2,)), dma, dma, dma((3,))],
        compiler_params=pltpu.CompilerParams(collective_id=0, has_side_effects=True, vmem_limit_bytes=16 << 20),
    )(*inputs)
    return pl.pallas_call(
        last_kernel,
        out_shape=jax.ShapeDtypeStruct(state.shape, jnp.float32),
        in_specs=[vmem],
        out_specs=anywhere,
        scratch_shapes=[
            pltpu.VMEM((2, faces, LANES, LANES), jnp.float32),
            pltpu.VMEM(state.shape, jnp.float32),
            dma((faces,)),
        ],
        compiler_params=pltpu.CompilerParams(vmem_limit_bytes=16 << 20),
    )(got)


def solution(mesh):
    groups, rows, columns = (mesh.shape[axis] for axis in ("face", "fy", "fx"))
    count = groups * rows * columns

    def body(*args):
        state = args[0]
        faces = state.shape[0]
        fits = rows == columns == 4 and 2 * count == HALF and faces * count <= LANES
        if fits and state.shape[1:] == (SIDE, SIDE, 3 * HALF) and 2 * faces <= SIDE:
            return by_level(groups, rows, *args)
        return per_device(*args)

    return jax.shard_map(
        body,
        mesh=mesh,
        in_specs=(
            P("face", "fy", "fx", None),
            P("face", "fy", "fx"),
            P(None, "face", "fy", "fx"),
            P("face", "fy", "fx"),
            P("face", "fy", "fx"),
            P(),
            P(),
        ),
        out_specs=P("face", "fy", "fx", None),
        check_vma=False,
    )
```

```python
import functools

import jax
import jax.numpy as jnp
import numpy as np
from jax import lax
from jax.experimental import pallas as pl
from jax.experimental.pallas import tpu as pltpu
from jax.sharding import PartitionSpec as P

time_step = 0.05
hyper_coeff = 0.0005
MESH = pl.DeviceIdType.MESH


def padded(cells, sides, width):
    for axis, dim in sides:
        count = lax.axis_size(axis)
        ends = count - 1
        head = lax.slice_in_dim(cells, 0, width, axis=dim)
        tail = lax.slice_in_dim(cells, cells.shape[dim] - width, cells.shape[dim], axis=dim)
        cells = jnp.concatenate(
            [
                lax.ppermute(tail, axis, [(i, (i + 1) % count) for i in range(ends)]),
                cells,
                lax.ppermute(head, axis, [((i + 1) % count, i) for i in range(ends)]),
            ],
            axis=dim,
        )
    return cells


def deriv_table():
    gll_nodes = np.array([-1.0, -1.0 / np.sqrt(5.0), 1.0 / np.sqrt(5.0), 1.0])
    bary_weights = np.ones(4)
    for j in range(4):
        for m in range(4):
            if m != j:
                bary_weights[j] = bary_weights[j] / (gll_nodes[j] - gll_nodes[m])
    matrix = np.zeros((4, 4))
    for i in range(4):
        for j in range(4):
            if i != j:
                matrix[i, j] = bary_weights[j] / bary_weights[i] / (gll_nodes[i] - gll_nodes[j])
        matrix[i, i] = -np.sum(matrix[i])
    return matrix


def along_x(values):
    face_count, row_count, col_count, chan_count = values.shape
    blocks = values.reshape(face_count, row_count, col_count // 4, 4, chan_count)
    result = jnp.einsum(
        "jk,abekc->abejc",
        jnp.asarray(deriv_table(), jnp.float32),
        blocks,
        precision=lax.Precision.HIGHEST,
    )
    return result.reshape(values.shape)


def along_y(values):
    face_count, row_count, col_count, chan_count = values.shape
    blocks = values.reshape(face_count, row_count // 4, 4, col_count, chan_count)
    result = jnp.einsum(
        "ik,aekxc->aeixc",
        jnp.asarray(deriv_table(), jnp.float32),
        blocks,
        precision=lax.Precision.HIGHEST,
    )
    return result.reshape(values.shape)


def mass_of(jacobian):
    weights = jnp.asarray([1.0 / 6.0, 5.0 / 6.0, 5.0 / 6.0, 1.0 / 6.0], jnp.float32)
    row_weight = jnp.tile(weights, jacobian.shape[1] // 4)
    col_weight = jnp.tile(weights, jacobian.shape[2] // 4)
    return jacobian * row_weight[None, :, None] * col_weight[None, None, :]


def tendency(state, geometry, planet):
    volume, metric_xx, metric_yy, metric_xy = geometry
    levels = state.shape[-1] // 3
    wind_u = state[..., :levels]
    wind_v = state[..., levels : 2 * levels]
    temper = state[..., 2 * levels :]
    contra_u = metric_xx * wind_u + metric_xy * wind_v
    contra_v = metric_xy * wind_u + metric_yy * wind_v
    energy = 0.5 * (wind_u * contra_u + wind_v * contra_v) + temper
    xderivs = along_x(jnp.concatenate([wind_v, temper, energy], -1))
    yderivs = along_y(jnp.concatenate([wind_u, temper, energy], -1))
    absolute = (xderivs[..., :levels] - yderivs[..., :levels]) / volume + planet
    tend_u = absolute * volume * contra_v - xderivs[..., 2 * levels :]
    tend_v = -absolute * volume * contra_u - yderivs[..., 2 * levels :]
    tend_t = -(
        contra_u * xderivs[..., levels : 2 * levels] + contra_v * yderivs[..., levels : 2 * levels]
    )
    return state + time_step * jnp.concatenate([tend_u, tend_v, tend_t], -1)


def laplace(values, geometry):
    volume, metric_xx, metric_yy, metric_xy = geometry
    grad_x = along_x(values)
    grad_y = along_y(values)
    flux_x = volume * (metric_xx * grad_x + metric_xy * grad_y)
    flux_y = volume * (metric_xy * grad_x + metric_yy * grad_y)
    return (along_x(flux_x) + along_y(flux_y)) / volume


def combine(values, axis):
    length = values.shape[axis] - 2
    positions = jnp.arange(length)
    leading = (positions % 4 == 0).astype(jnp.float32)
    trailing = (positions % 4 == 3).astype(jnp.float32)
    broad_shape = [1, 1, 1, 1]
    broad_shape[axis] = length
    leading = leading.reshape(broad_shape)
    trailing = trailing.reshape(broad_shape)
    middle = lax.slice_in_dim(values, 1, length + 1, axis=axis)
    previous = lax.slice_in_dim(values, 0, length, axis=axis)
    following = lax.slice_in_dim(values, 2, length + 2, axis=axis)
    return middle + leading * previous + trailing * following


def rotate(segment, quarter, levels):
    cosine = ((quarter == 0).astype(jnp.float32) - (quarter == 2).astype(jnp.float32))[..., None]
    sine_part = ((quarter == 1).astype(jnp.float32) - (quarter == 3).astype(jnp.float32))[..., None]
    wind_u = segment[..., :levels]
    wind_v = segment[..., levels : 2 * levels]
    return jnp.concatenate(
        [
            cosine * wind_u - sine_part * wind_v,
            sine_part * wind_u + cosine * wind_v,
            segment[..., 2 * levels :],
        ],
        -1,
    )


def in_face(values):
    across = combine(padded(values, (("fx", 2),), 1), 2)
    return combine(padded(across, (("fy", 1),), 1), 1)


def place_pieces(
    got_flat,
    got_tall,
    vector,
    nbr_edge,
    flat_edge,
    tall_edge,
    on_south,
    on_west,
    flat_start,
    tall_start,
    face_local,
    side_nodes,
    chan_count,
    levels,
):
    edge_ids = jnp.arange(4, dtype=jnp.int32)
    flat_target = nbr_edge[:, flat_edge]
    tall_target = nbr_edge[:, tall_edge]
    if vector:
        got_flat = rotate(got_flat, ((flat_target - flat_edge + 2) % 4)[None, :, None], levels)
        got_tall = rotate(got_tall, ((tall_target - tall_edge + 2) % 4)[None, :, None], levels)
    got_flat = jnp.where(on_south, got_flat[:, :, ::-1], got_flat)
    got_tall = jnp.where(on_west, got_tall, got_tall[:, :, ::-1])
    flat_pick = (flat_target[:, None] == edge_ids[None, :]).astype(jnp.float32)
    tall_pick = (tall_target[:, None] == edge_ids[None, :]).astype(jnp.float32)
    flat_rims = jnp.einsum("se,gsjc->gejc", flat_pick, got_flat, precision=lax.Precision.HIGHEST)
    tall_rims = jnp.einsum("se,gsjc->gejc", tall_pick, got_tall, precision=lax.Precision.HIGHEST)
    empty_rims = jnp.zeros((face_local, 4, side_nodes, chan_count), jnp.float32)
    rim_strips = lax.dynamic_update_slice(empty_rims, flat_rims, (0, 0, flat_start, 0))
    return rim_strips + lax.dynamic_update_slice(empty_rims, tall_rims, (0, 0, tall_start, 0))


def outgoing(
    summed, nbr_face, face_ids, flat_edge, tall_edge, on_south, on_west, flat_live, tall_live
):
    row_count = summed.shape[1]
    col_count = summed.shape[2]
    all_faces = jnp.arange(nbr_face.shape[0], dtype=jnp.int32)
    flat_piece = jnp.where(on_south, summed[:, 0], summed[:, row_count - 1])
    tall_piece = jnp.where(on_west, summed[:, :, 0], summed[:, :, col_count - 1])
    flat_dest = nbr_face[face_ids, flat_edge]
    tall_dest = nbr_face[face_ids, tall_edge]
    flat_send = ((all_faces[:, None] == flat_dest[None, :]) & flat_live).astype(jnp.float32)
    tall_send = ((all_faces[:, None] == tall_dest[None, :]) & tall_live).astype(jnp.float32)
    return (
        flat_send[:, :, None, None] * flat_piece[None],
        tall_send[:, :, None, None] * tall_piece[None],
    )


def assemble(values, vector, nbr_face, nbr_edge):
    summed = in_face(values)
    face_local, row_count, col_count, chan_count = summed.shape
    levels = chan_count // 3
    row_index = lax.axis_index("fy")
    col_index = lax.axis_index("fx")
    side_nodes = row_count * lax.axis_size("fy")
    face_ids = lax.axis_index("face") * face_local + jnp.arange(face_local, dtype=jnp.int32)
    on_south = row_index == 0
    on_north = row_index == lax.axis_size("fy") - 1
    on_west = col_index == 0
    on_east = col_index == lax.axis_size("fx") - 1
    flat_live = on_south | on_north
    tall_live = on_west | on_east
    flat_edge = jnp.where(on_south, 0, 2).astype(jnp.int32)
    tall_edge = jnp.where(on_west, 3, 1).astype(jnp.int32)
    flat_start = jnp.where(
        on_south, side_nodes - (col_index + 1) * col_count, col_index * col_count
    )
    tall_start = jnp.where(on_west, row_index * row_count, side_nodes - (row_index + 1) * row_count)
    send_flat, send_tall = outgoing(
        summed, nbr_face, face_ids, flat_edge, tall_edge, on_south, on_west, flat_live, tall_live
    )
    got_flat, got_tall = (
        lax.all_to_all(send_flat, "face", split_axis=0, concat_axis=1, tiled=True),
        lax.all_to_all(send_tall, "face", split_axis=0, concat_axis=1, tiled=True),
    )
    rim_strips = place_pieces(
        got_flat,
        got_tall,
        vector,
        nbr_edge,
        flat_edge,
        tall_edge,
        on_south,
        on_west,
        flat_start,
        tall_start,
        face_local,
        side_nodes,
        chan_count,
        levels,
    )
    flat_lines = jnp.stack([rim_strips[:, 0], rim_strips[:, 2, ::-1]], axis=1)
    flat_lines = flat_lines.reshape(face_local, 2, lax.axis_size("fx"), col_count, chan_count)
    tall_lines = jnp.stack([rim_strips[:, 1], rim_strips[:, 3, ::-1]], axis=1)
    tall_lines = tall_lines.reshape(face_local, 2, lax.axis_size("fy"), row_count, chan_count)
    flat_whole = lax.psum(flat_lines, "fy")
    tall_whole = lax.psum(tall_lines, "fx")
    flat_block = lax.psum_scatter(flat_whole, "fx", scatter_dimension=2, tiled=True)
    tall_block = lax.psum_scatter(tall_whole, "fy", scatter_dimension=2, tiled=True)
    flat_add = jnp.where(on_south, flat_block[:, 0, 0], flat_block[:, 1, 0])
    tall_add = jnp.where(on_west, tall_block[:, 1, 0], tall_block[:, 0, 0])
    result = summed.at[:, 0].add(jnp.where(on_south, flat_add, 0.0))
    result = result.at[:, row_count - 1].add(jnp.where(on_north, flat_add, 0.0))
    result = result.at[:, :, 0].add(jnp.where(on_west, tall_add, 0.0))
    result = result.at[:, :, col_count - 1].add(jnp.where(on_east, tall_add, 0.0))
    return result


def per_device(state, jacobian, metric_diag, metric_cross, coriolis, nbr_face, nbr_edge):
    node_mass = mass_of(jacobian)[..., None]
    total_mass = assemble(node_mass, False, nbr_face, nbr_edge)
    geometry = (
        jacobian[..., None],
        metric_diag[0][..., None],
        metric_diag[1][..., None],
        metric_cross[..., None],
    )
    raw = tendency(state, geometry, coriolis[..., None])
    sectioned = assemble(node_mass * raw, True, nbr_face, nbr_edge) / total_mass
    first_lap = (
        assemble(node_mass * laplace(sectioned, geometry), True, nbr_face, nbr_edge) / total_mass
    )
    second_lap = (
        assemble(node_mass * laplace(first_lap, geometry), True, nbr_face, nbr_edge) / total_mass
    )
    return sectioned - hyper_coeff * second_lap


SIDE = 8
HALF = 64
LANES = 128


IN_KINDS = "gggtttwwwgtw"
IN_COLUMNS = ("321321321000", "320320320111", "301301301222", "012012012333")


def up(v, count, axis):
    return pltpu.roll(v, v.shape[axis] - count, axis)


def down(v, count, axis):
    return pltpu.roll(v, count, axis)


def slope(a):
    d = deriv_table()
    p0, p1, m0, m1 = a[0] + a[3], a[1] + a[2], a[0] - a[3], a[1] - a[2]
    bend = p0 - p1
    o0 = jnp.float32((d[0, 0] + d[0, 3]) / 2) * bend
    o1 = jnp.float32((d[1, 0] + d[1, 3]) / 2) * bend
    q0 = jnp.float32((d[0, 0] - d[0, 3]) / 2) * m0 + jnp.float32((d[0, 1] - d[0, 2]) / 2) * m1
    q1 = jnp.float32((d[1, 0] - d[1, 3]) / 2) * m0 + jnp.float32((d[1, 1] - d[1, 2]) / 2) * m1
    return [q0 + o0, q1 + o1, q1 - o1, q0 - o0]


def slope_x(v):
    return [slope(v[i]) for i in range(4)]


def slope_y(v):
    cols = [slope([v[i][j] for i in range(4)]) for j in range(4)]
    return [[cols[j][i] for j in range(4)] for i in range(4)]


def spread(mix, plane, er, i, which, v):
    for ec in range(2):
        mix[plane, pl.ds(er * 64 + ec * 32 + which * 16 + i * 4, 4), :] = v[4 * ec : 4 * ec + 4]


def by_node(mix, plane):
    return jnp.concatenate([mix[plane, pl.ds(n, 8, stride=16), :] for n in range(16)], axis=0)


def main_kernel(
    groups,
    blocks,
    nbr_face_in,
    nbr_edge_in,
    state_in,
    jac_in,
    diag_in,
    cross_in,
    coriolis_in,
    out,
    nbr_face,
    nbr_edge,
    state,
    jac,
    diag,
    cross,
    coriolis,
    mix,
    send,
    send_geo,
    got,
    got_geo,
    coef,
    section,
    back,
    sem_load,
    sem_s_geo,
    sem_r_geo,
    sem_s_in,
    sem_r_in,
    sem_s_out,
    sem_r_out,
    sem_own,
):
    faces = state.shape[0]
    count = groups * blocks * blocks
    last = blocks - 1
    g = lax.axis_index("face")
    y = lax.axis_index("fy")
    x = lax.axis_index("fx")
    me = (g * blocks + y) * blocks + x

    def by_distance(at):
        return [last - at, lax.rem(at + 2, 4), at + 1 - 2 * lax.rem(at, 2), at]

    def others(columns):
        for n, tx in enumerate(columns):
            for ty in by_distance(y)[: blocks - 1] + [y]:
                for tg in (lax.rem(g + 1, groups), g):
                    if tx is not x or ty is not y or tg is not g:
                        yield (tg * blocks + ty) * blocks + tx, (tg, ty, tx)

    def towards(columns):
        for tx in columns:
            for ty in range(blocks):
                for tg in range(groups):
                    yield (tg * blocks + ty) * blocks + tx, (tg, ty, tx)

    loads = [
        pltpu.make_async_copy(src, dst, sem_load.at[n])
        for n, (src, dst) in enumerate(
            (
                (state_in, state),
                (jac_in, jac),
                (diag_in, diag),
                (cross_in, cross),
                (coriolis_in, coriolis),
                (nbr_face_in, nbr_face),
                (nbr_edge_in, nbr_edge),
            )
        )
    ]
    barrier = pltpu.get_barrier_semaphore()
    for _, at in others(by_distance(x)):
        pl.semaphore_signal(barrier, inc=1, device_id=at, device_id_type=MESH)
    for load in loads:
        load.start()
    for load in loads[1:]:
        load.wait()

    sub = lax.broadcasted_iota(jnp.int32, (SIDE, LANES), 0)
    lane = lax.broadcasted_iota(jnp.int32, (SIDE, LANES), 1)
    low = lane < HALF
    node = sub % 4
    table = deriv_table()
    weights = (1.0 / 6.0, 5.0 / 6.0, 5.0 / 6.0, 1.0 / 6.0)
    zero = jnp.zeros((SIDE, LANES), jnp.float32)

    def per_node(entries, at):
        total = jnp.full(at.shape, entries[0], jnp.float32)
        for n in range(1, 4):
            total = jnp.where(at == n, jnp.float32(entries[n]), total)
        return total

    taps = {
        s: per_node([float(table[n, n + s]) if 0 <= n + s < 4 else 0.0 for n in range(4)], node)
        for s in range(-3, 4)
    }

    def swap(v):
        return pltpu.roll(v, HALF, 1)

    def along_sub(v):
        total = taps[0] * v
        for s in (-3, -2, -1, 1, 2, 3):
            total = total + taps[s] * pltpu.roll(v, (-s) % SIDE, 0)
        return total

    def pick(v, at):
        return jnp.take_along_axis(v, at, axis=1, mode="promise_in_bounds")

    def spread_lanes(tiles):
        tiles = tiles + [tiles[0]] * (LANES // SIDE - len(tiles))
        return jnp.concatenate(tiles, axis=0).T

    tile_sub = lax.broadcasted_iota(jnp.int32, (SIDE, SIDE), 0) % 4
    tile_lane = lax.broadcasted_iota(jnp.int32, (SIDE, SIDE), 1) % 4
    tile_weight = per_node(weights, tile_sub) * per_node(weights, tile_lane)
    near_tiles, far_tiles = [], []
    for f in range(faces):
        vol, m_xx, m_yy, m_xy = jac[f], diag[0, f], diag[1, f], cross[f]
        mass = vol * tile_weight
        near_tiles += [m_xx, m_yy, m_xy, vol * coriolis[f], mass]
        far_tiles += [vol * m_xx, vol * m_yy, vol * m_xy, mass]
    local, shared = spread_lanes(near_tiles), spread_lanes(far_tiles)

    def spot(f, k, r):
        return (f * 5 + k) * SIDE + r

    cells = [(f, r) for f in range(faces) for r in range(SIDE)]
    lines = [[n + i for i in range(4)] for n in range(0, len(cells), 4)]
    for r in range(SIDE):
        for h in range(2):
            at = (lane // 2 % faces) * (4 * SIDE) + (2 * h + lane % 2) * SIDE + r
            spread(mix, faces, r // 4, r % 4, h, pick(shared, at))
    own = [pick(local, jnp.where(low, spot(f, 0, r), spot(f, 1, r))) for f, r in cells]
    skew = [pick(local, lane * 0 + spot(f, 2, r)) for f, r in cells]
    turn = [pick(local, lane * 0 + spot(f, 3, r)) for f, r in cells]
    mass = [pick(local, lane * 0 + spot(f, 4, r)) for f, r in cells]
    send_geo[...] = by_node(mix, faces).T[0:SIDE]
    loads[0].wait()
    wind = [state[f, r, :, 0 : 2 * HALF] for f, r in cells]
    temp = [state[f, r, :, 2 * HALF : 3 * HALF] for f, r in cells]
    temp = [jnp.concatenate([t, t], axis=1) for t in temp]
    other = [swap(w) for w in wind]
    contra = [m * w + n * o for m, n, w, o in zip(own, skew, wind, other)]
    power = [w * c for w, c in zip(wind, contra)]
    crossed = [swap(c) for c in contra]
    turned = [swap(p) for p in power]
    energy = [0.5 * (p + q) + t for p, q, t in zip(power, turned, temp)]

    def down_lines(v):
        out = [None] * len(cells)
        for line in lines:
            for n, d in zip(line, slope([v[n] for n in line])):
                out[n] = d
        return out

    dxs = [along_sub(jnp.where(low, e, w)) for e, w in zip(energy, wind)]
    dys = down_lines([jnp.where(low, w, e) for e, w in zip(energy, wind)])
    flow = [c * jnp.where(low, a, b) for c, a, b in zip(contra, [along_sub(t) for t in temp], down_lines(temp))]
    dxv = [swap(a) for a in dxs]
    dyu = [swap(a) for a in dys]
    flow = [q + swap(q) for q in flow]
    heat = [m * (t - time_step * q) for m, t, q in zip(mass, temp, flow)]
    fresh = []
    for n in range(len(cells)):
        spin = jnp.where(low, dxv[n] - dys[n], dyu[n] - dxs[n]) + jnp.where(low, turn[n], -turn[n])
        tend = spin * crossed[n] - jnp.where(low, dxs[n], dys[n])
        fresh.append(mass[n] * (wind[n] + time_step * tend))
    second = (lane >= 32) & (lane < 64)
    shifted = [(down(t, 32, 1), up(w, 32, 1)) for t, w in zip(heat, fresh)]
    for n, (f, r) in enumerate(cells):
        spread(mix, f, r // 4, r % 4, 0, jnp.where(second, shifted[n][0], fresh[n]))
        spread(mix, f, r // 4, r % 4, 1, jnp.where(second, heat[n], shifted[n][1]))
    for f in range(faces):
        turned = by_node(mix, f).T
        for k, part in enumerate((0, 2, 1)):
            send[k * faces + f] = turned[part * count : (part + 1) * count]

    er, ec, lev = sub // 4, (sub // 2) % 2, sub % 2
    lx, ly = lane % blocks, (lane // blocks) % blocks
    panel = lane // (blocks * blocks)
    er0, er1, ec0, ec1 = er == 0, er == 1, ec == 0, ec == 1
    x_lo, x_hi, y_lo, y_hi = lx == 0, lx == last, ly == 0, ly == last
    edge_at = (er0 & y_lo, er1 & x_hi, er0 & y_hi, er1 & x_lo)

    first_at = jnp.zeros((SIDE, LANES), jnp.int32)
    step_at, quarter_at = first_at, first_at
    for e in range(4):
        firsts, steps, quarters = first_at * 0, first_at * 0, first_at * 0
        for f in range(faces):
            for k in range(groups):
                nf = nbr_face[e, k * faces + f]
                ne = nbr_edge[e, k * faces + f]
                nl, ng = nf % faces, nf // faces
                tall = ne % 2
                step = 1 + tall * (blocks - 1)
                flips = jnp.where(ne >= 2, 0 if e < 2 else 1, 1 if e < 2 else 0)
                offset = jnp.where(ne == 2, last * blocks, jnp.where(ne == 1, last, 0))
                first = (nl * groups + ng) * (blocks * blocks) + offset + flips * (last * step)
                here = panel == f * groups + k
                firsts = jnp.where(here, first, firsts)
                steps = jnp.where(here, step * (1 - 2 * flips), steps)
                quarters = jnp.where(here, (e - ne + 2 + 4) % 4, quarters)
        first_at = jnp.where(edge_at[e], firsts, first_at)
        step_at = jnp.where(edge_at[e], steps, step_at)
        quarter_at = jnp.where(edge_at[e], quarters, quarter_at)
    source_at = first_at + step_at * jnp.where(er0, lx, ly)
    flipped = step_at < 0
    from_flat = (step_at == 1) | (step_at == -1)
    cosine = jnp.where(quarter_at == 0, 1.0, jnp.where(quarter_at == 2, -1.0, 0.0))
    sine = jnp.where(quarter_at == 1, 1.0, jnp.where(quarter_at == 3, -1.0, 0.0))

    def next_row(v):
        s = down(v, 4, 0)
        return jnp.where(er0, s, jnp.where(y_hi, zero, up(s, blocks, 1)))

    def prev_row(v):
        s = down(v, 4, 0)
        return jnp.where(er1, s, jnp.where(y_lo, zero, down(s, blocks, 1)))

    def next_col(v):
        return jnp.where(ec0, up(v, 2, 0), jnp.where(x_hi, zero, up(down(v, 2, 0), 1, 1)))

    def prev_col(v):
        return jnp.where(ec1, down(v, 2, 0), jnp.where(x_lo, zero, down(up(v, 2, 0), 1, 1)))

    def rims(v):
        found = []
        for b in range(4):
            flat = jnp.where(y_hi, v[3][b], v[0][b])
            flat = jnp.where(er0 == y_hi, down(flat, 4, 0), flat)
            tall = jnp.where(x_hi, v[b][3], v[b][0])
            tall = jnp.where(ec0 == x_hi, jnp.where(x_hi, up(tall, 2, 0), down(tall, 2, 0)), tall)
            tall = jnp.where(er == ec, tall, down(tall, 4, 0))
            found.append(jnp.where(from_flat, pick(flat, source_at), pick(tall, source_at)))
        partner = []
        for b in range(4):
            w = found[3 - b]
            w = jnp.where(ec0, up(w, 2, 0), down(w, 2, 0))
            partner.append(jnp.where(flipped, w, found[b]))
        return partner

    def glue(v, partner):
        v = [list(row) for row in v]
        sides = []
        for j in range(4):
            a, b, p = v[0][j], v[3][j], partner[j]
            s = down(p, 4, 0)
            v[0][j] = a + jnp.where(edge_at[0], p, prev_row(b))
            v[3][j] = b + jnp.where(er1 & y_hi, s, next_row(a))
            q = jnp.where(er1, p, s)
            q = jnp.where(er == ec, q, jnp.where(er0, down(q, 2, 0), up(q, 2, 0)))
            sides.append(q)
        q0, q3 = sides[0], sides[3]
        sides[0], sides[3] = q0 + prev_row(q3), q3 + next_row(q0)
        for i in range(4):
            a, b, q = v[i][0], v[i][3], sides[i]
            v[i][0] = a + jnp.where(ec0 & x_lo, q, prev_col(b))
            v[i][3] = b + jnp.where(ec1 & x_hi, q, next_col(a))
        return v

    def assemble_one(v):
        return glue(v, rims(v))

    def assemble_pair(u, v):
        pu, pv = rims(u), rims(v)
        tu = [cosine * a - sine * b for a, b in zip(pu, pv)]
        tv = [sine * a + cosine * b for a, b in zip(pu, pv)]
        return glue(u, tu), glue(v, tv)

    def grid(flat):
        return [[flat[8 * (4 * i + j) : 8 * (4 * i + j) + 8] for j in range(4)] for i in range(4)]

    def receive(ref, planes):
        blocks_in = [ref[p] for p in planes]
        blocks_in += [blocks_in[0]] * (LANES // count - len(blocks_in))
        return grid(jnp.concatenate(blocks_in, axis=0).T)

    def put(ref, k, v):
        for i in range(4):
            for j in range(4):
                ref[k, i, j] = v[i][j]

    def take(ref, k):
        return [[ref[k, i, j] for j in range(4)] for i in range(4)]

    def each(fn, *vs):
        return [[fn(*(v[i][j] for v in vs)) for j in range(4)] for i in range(4)]

    def copy_to(at, src, dst, sem_s, sem_r):
        pltpu.make_async_remote_copy(
            src_ref=src,
            dst_ref=dst,
            send_sem=sem_s,
            recv_sem=sem_r,
            device_id=at,
            device_id_type=MESH,
        ).start()

    def all_of(ref, sem_s, sem_r, first=0, planes=None, rows=None):
        planes = ref.shape[0] if planes is None else planes
        part = ref.at[pl.ds(first, planes), pl.ds(0, rows or count - 1)]
        return pltpu.make_async_remote_copy(
            src_ref=part,
            dst_ref=part,
            send_sem=sem_s,
            recv_sem=sem_r,
            device_id=(g, y, lax.rem(x + 1, blocks)),
            device_id_type=MESH,
        )

    pairs = 2 * faces
    half = count // 2
    parts = ((2 * faces, faces), (0, 2 * faces))
    pl.semaphore_wait(barrier, count - 1)
    odd = lax.rem(y, 2) == 1
    even = jnp.logical_not(odd)

    def send_shapes(c):
        for d, at in towards([c]):
            if at[1] % 2 == 1:
                src, dst = send_geo.at[pl.ds(0, pairs)], got_geo.at[:, me]
                pl.when(d != me)(functools.partial(copy_to, at, src, dst, sem_s_geo.at[0], sem_r_geo.at[0]))

    def send_part(n, c):
        part = pl.ds(*parts[n])
        for d, at in towards([c]):
            src, dst = send.at[part, d], got.at[part, me]
            pl.when(d != me)(functools.partial(copy_to, at, src, dst, sem_s_in.at[n], sem_r_in.at[n]))

    def send_from(column):
        for kind, c in zip(IN_KINDS, map(int, IN_COLUMNS[column])):
            if kind == "g":
                send_shapes(c)
            else:
                send_part("tw".index(kind), c)

    for column in range(blocks):
        pl.when(x == column)(functools.partial(send_from, column))

    for q in range(3 * faces):
        got[q, pl.ds(me, 1), :] = send[q, pl.ds(me, 1), :]

    @pl.when(odd)
    def _():
        for q in range(pairs):
            got_geo[q, pl.ds(me, 1), :] = send_geo[pl.ds(q, 1), :]


    relay = pltpu.make_async_remote_copy(
        src_ref=got_geo,
        dst_ref=got_geo,
        send_sem=sem_s_geo.at[1],
        recv_sem=sem_r_geo.at[1],
        device_id=(g, y + 1 - 2 * lax.rem(y, 2), x),
        device_id_type=MESH,
    )

    def shapes(rows):
        return all_of(got_geo, sem_s_geo.at[0], sem_r_geo.at[0], rows=rows)

    @pl.when(odd)
    def _():
        shapes(count - 1).wait_recv()
        relay.start()

    pl.when(even)(relay.wait_recv)
    for p in range(2):
        both = receive(got_geo, range(p, pairs, 2))
        put(coef, 2 * p, each(lambda v: jnp.where(lev == 0, v, down(v, 1, 0)), both))
        put(coef, 2 * p + 1, each(lambda v: jnp.where(lev == 1, v, up(v, 1, 0)), both))
    put(coef, 3, each(lambda v: 1.0 / v, assemble_one(take(coef, 3))))

    def fields_in(k):
        return receive(got, range(k * faces, (k + 1) * faces))

    def scaled(v):
        return each(lambda a, b: a * b, v, take(coef, 3))

    def laplace_of(v):
        a, b, c = take(coef, 0), take(coef, 1), take(coef, 2)
        gx, gy = slope_x(v), slope_y(v)
        fx = each(lambda p, q, m, n: m * p + n * q, gx, gy, a, b)
        fy = each(lambda p, q, m, n: m * p + n * q, gx, gy, b, c)
        total = each(lambda p, q: p + q, slope_x(fx), slope_y(fy))
        return [[jnp.float32(weights[i] * weights[j]) * total[i][j] for j in range(4)] for i in range(4)]

    def finish(k, v):
        done = each(lambda s, a: s - hyper_coeff * a, take(section, k), v)
        turned = jnp.concatenate([done[i][j] for i in range(4) for j in range(4)], axis=0).T
        for f in range(faces):
            back[k * faces + f] = turned[f * count : (f + 1) * count]

    def send_back(n):
        part = pl.ds(*parts[n])
        for d, at in towards(range(blocks)):
            pl.when(d != me)(
                functools.partial(copy_to, at, back.at[part, d], out.at[part, me], sem_s_out, sem_r_out)
            )

    def kept(n):
        part = pl.ds(*parts[n])
        return pltpu.make_async_copy(back.at[part, me], out.at[part, me], sem_own.at[n])

    def arrived(n):
        first, planes = parts[n]
        return all_of(got, sem_s_in.at[n], sem_r_in.at[n], first, planes)

    arrived(0).wait_recv()
    heat = scaled(assemble_one(fields_in(2)))
    put(section, 2, heat)
    heat = scaled(assemble_one(laplace_of(heat)))
    heat = scaled(assemble_one(laplace_of(heat)))
    finish(2, heat)
    send_back(0)
    kept(0).start()
    arrived(1).wait_recv()
    wind_u, wind_v = assemble_pair(fields_in(0), fields_in(1))
    put(section, 0, scaled(wind_u))
    put(section, 1, scaled(wind_v))
    wind_u, wind_v = assemble_pair(laplace_of(take(section, 0)), laplace_of(take(section, 1)))
    wind_u, wind_v = assemble_pair(laplace_of(scaled(wind_u)), laplace_of(scaled(wind_v)))
    finish(0, scaled(wind_u))
    finish(1, scaled(wind_v))
    send_back(1)
    kept(1).start()

    @pl.when(odd)
    def _():
        shapes(half - 1).wait_send()
        relay.wait_send()

    pl.when(even)(shapes(half).wait_send)
    arrived(0).wait_send()
    arrived(1).wait_send()
    kept(0).wait()
    kept(1).wait()
    all_of(out, sem_s_out, sem_r_out).wait_send()
    all_of(out, sem_s_out, sem_r_out).wait_recv()


def last_kernel(got, out, mix, full, sem):
    faces = full.shape[0]
    lane = lax.broadcasted_iota(jnp.int32, (SIDE, LANES), 1)
    first = (lane // 32) % 2 == 0

    widths = 2 * HALF, HALF

    def half_rows(n, f, r, h):
        start = (r % 4) * 32 + (r // 4) * 4 + h
        return jnp.concatenate([mix[n, f, pl.ds(start + ec * 2, 4, stride=8), 0 : widths[n]] for ec in range(2)], axis=0)

    def copy_of(f):
        return pltpu.make_async_copy(full.at[f], out.at[f], sem.at[f])

    for f in range(faces):
        u, v, t = (got[k * faces + f] for k in range(3))
        for m, parts in enumerate(((u, u, v, v), (t, t))):
            mix[m, f, :, 0 : widths[m]] = jnp.concatenate(parts, axis=0).T
    for f in range(faces):
        for r in range(SIDE):
            wind, temp = (
                jnp.where(first[:, 0 : widths[m]], half_rows(m, f, r, 0), half_rows(m, f, r, 1)) for m in range(2)
            )
            full[f, r, :, 0 : 2 * HALF] = wind
            full[f, r, :, 2 * HALF : 3 * HALF] = temp
        copy_of(f).start()
    for f in range(faces):
        copy_of(f).wait()


def by_level(groups, blocks, state, jacobian, metric_diag, metric_cross, coriolis, nbr_face, nbr_edge):
    faces = state.shape[0]
    count = groups * blocks * blocks
    vmem, anywhere = pl.BlockSpec(memory_space=pltpu.VMEM), pl.BlockSpec(memory_space=pl.ANY)
    inputs = (nbr_face.T, nbr_edge.T, state, jacobian, metric_diag, metric_cross, coriolis)
    inputs = [pltpu.with_memory_space_constraint(a, pltpu.HBM) for a in inputs]
    piece = (3 * faces, count, LANES)
    cells = (4, 4, SIDE, LANES)
    dma = pltpu.SemaphoreType.DMA
    got = pl.pallas_call(
        functools.partial(main_kernel, groups, blocks),
        out_shape=jax.ShapeDtypeStruct(piece, jnp.float32),
        in_specs=[pl.BlockSpec(memory_space=pltpu.HBM)] * 7,
        out_specs=anywhere,
        scratch_shapes=[pltpu.SMEM(a.shape, a.dtype) for a in inputs[:2]]
        + [pltpu.VMEM(a.shape, a.dtype) for a in inputs[2:]]
        + [
            pltpu.VMEM((faces + 1, LANES, LANES), jnp.float32),
            pltpu.VMEM(piece, jnp.float32),
            pltpu.VMEM((SIDE, LANES), jnp.float32),
            pltpu.VMEM(piece, jnp.float32),
            pltpu.VMEM((2 * faces, count, LANES), jnp.float32),
            pltpu.VMEM((4,) + cells, jnp.float32),
            pltpu.VMEM((3,) + cells, jnp.float32),
            pltpu.VMEM(piece, jnp.float32),
        ]
        + [dma((7,)), dma((2,)), dma((2,)), dma((2,)), dma((2,)), dma, dma, dma((3,))],
        compiler_params=pltpu.CompilerParams(collective_id=0, has_side_effects=True, vmem_limit_bytes=16 << 20),
    )(*inputs)
    return pl.pallas_call(
        last_kernel,
        out_shape=jax.ShapeDtypeStruct(state.shape, jnp.float32),
        in_specs=[vmem],
        out_specs=anywhere,
        scratch_shapes=[
            pltpu.VMEM((2, faces, LANES, LANES), jnp.float32),
            pltpu.VMEM(state.shape, jnp.float32),
            dma((faces,)),
        ],
        compiler_params=pltpu.CompilerParams(vmem_limit_bytes=16 << 20),
    )(got)


def solution(mesh):
    groups, rows, columns = (mesh.shape[axis] for axis in ("face", "fy", "fx"))
    count = groups * rows * columns

    def body(*args):
        state = args[0]
        faces = state.shape[0]
        fits = rows == columns == 4 and 2 * count == HALF and faces * count <= LANES
        if fits and state.shape[1:] == (SIDE, SIDE, 3 * HALF) and 2 * faces <= SIDE:
            return by_level(groups, rows, *args)
        return per_device(*args)

    return jax.shard_map(
        body,
        mesh=mesh,
        in_specs=(
            P("face", "fy", "fx", None),
            P("face", "fy", "fx"),
            P(None, "face", "fy", "fx"),
            P("face", "fy", "fx"),
            P("face", "fy", "fx"),
            P(),
            P(),
        ),
        out_specs=P("face", "fy", "fx", None),
        check_vma=False,
    )
```
